8 devices in a mesh: bx: 2 (over z, y), sq: 4 (over x, core).
Axes of the slice: x: 2, y: 2, z: 1, core: 2. Of those that a mesh axis runs over, the one named last changes fastest.
Arguments:
- hidden: bfloat16 [128, 2048], P('bx'), parts along dimension 0
- w_query: bfloat16 [2048, 2048], P(None, 'sq')
- w_key: bfloat16 [2048, 128], replicated
- w_value: bfloat16 [2048, 128], replicated
- w_out: bfloat16 [2048, 2048], P('sq')
- k_cache: bfloat16 [128, 8192, 128], P('bx', 'sq'), parts along dimension 0
- v_cache: bfloat16 [128, 8192, 128], P('bx', 'sq'), parts along dimension 0
- lengths: int32 [128], P('bx'), parts along dimension 0
Outputs:
- output 1: bfloat16 [128, 2048], P('bx', 'sq'), parts along dimension 0
- output 2: bfloat16 [128, 128], P('bx'), parts along dimension 0
- output 3: bfloat16 [128, 128], P('bx'), parts along dimension 0
There are 2 independent parts. The reference program is written for one: setup_inputs(seed, part) draws one part's arguments, and reference() takes and returns one part's arrays. A program takes and returns all parts, laid end to end along the dimension named above; an argument that names none is the same for every part.
All inputs are finite; a program needn't handle non-finite values.
Results may differ from the reference program's by a relative error of at most 0.00560568.
Values sent between devices are 32-bit elements.
A program may use at most 1 GiB of HBM per device.

```python
import jax
import jax.numpy as jnp
from jax import lax

BATCH_ROWS = 64
SEQ_LEN = 8192
EMBED_DIM = 2048
NUM_HEADS = 16
HEAD_DIM = 128


def rope_tables(lengths):
    half_dim = HEAD_DIM // 2
    inv_freq = 10000.0 ** (-jnp.arange(half_dim, dtype=jnp.float32) * 2.0 / HEAD_DIM)
    angles = lengths.astype(jnp.float32)[:, None] * inv_freq[None, :]
    return jnp.cos(angles), jnp.sin(angles)


def apply_rope(x_val, cos_t, sin_t):
    half_dim = x_val.shape[-1] // 2
    x_low = x_val[..., :half_dim]
    x_high = x_val[..., half_dim:]
    return jnp.concatenate([x_low * cos_t - x_high * sin_t, x_high * cos_t + x_low * sin_t], axis=-1)


def setup_inputs(seed: int = 0, part: int = 0) -> dict:
    part_key = jax.random.fold_in(jax.random.key(seed), part)
    key_list = jax.random.split(part_key, 6)
    weight_keys = jax.random.split(jax.random.key(seed + 1), 4)
    q_cols = NUM_HEADS * HEAD_DIM
    cache_shape = (BATCH_ROWS, SEQ_LEN, HEAD_DIM)
    hidden = jax.random.normal(key_list[0], (BATCH_ROWS, EMBED_DIM), jnp.float32)
    w_query = jax.random.normal(weight_keys[0], (EMBED_DIM, q_cols), jnp.float32) * (2.0 * EMBED_DIM ** -0.5)
    w_key = jax.random.normal(weight_keys[1], (EMBED_DIM, HEAD_DIM), jnp.float32) * EMBED_DIM ** -0.5
    w_value = jax.random.normal(weight_keys[2], (EMBED_DIM, HEAD_DIM), jnp.float32) * EMBED_DIM ** -0.5
    w_out = jax.random.normal(weight_keys[3], (q_cols, EMBED_DIM), jnp.float32) * q_cols ** -0.5
    walk_k = jnp.cumsum(jax.random.normal(key_list[1], cache_shape, jnp.float32), axis=1) * (1.5 * SEQ_LEN ** -0.5)
    k_cache = jax.random.normal(key_list[2], cache_shape, jnp.float32) + walk_k
    walk_v = jnp.cumsum(jax.random.normal(key_list[3], cache_shape, jnp.float32), axis=1) * SEQ_LEN ** -0.5
    v_cache = 0.5 * jax.random.normal(key_list[4], cache_shape, jnp.float32) + walk_v
    lengths = jax.random.randint(key_list[5], (BATCH_ROWS,), SEQ_LEN // 4, SEQ_LEN, dtype=jnp.int32)
    lengths = lengths.at[0].set(SEQ_LEN - 1)
    return {
        'hidden': hidden.astype(jnp.bfloat16),
        'w_query': w_query.astype(jnp.bfloat16),
        'w_key': w_key.astype(jnp.bfloat16),
        'w_value': w_value.astype(jnp.bfloat16),
        'w_out': w_out.astype(jnp.bfloat16),
        'k_cache': k_cache.astype(jnp.bfloat16),
        'v_cache': v_cache.astype(jnp.bfloat16),
        'lengths': lengths,
    }


def reference(hidden, w_query, w_key, w_value, w_out, k_cache, v_cache, lengths):
    q_cols = NUM_HEADS * HEAD_DIM
    cos_t, sin_t = rope_tables(lengths)
    q_proj = jnp.dot(hidden, w_query, preferred_element_type=jnp.float32).reshape(BATCH_ROWS, NUM_HEADS, HEAD_DIM)
    q_rot = apply_rope(q_proj, cos_t[:, None, :], sin_t[:, None, :]).astype(jnp.bfloat16)
    k_new = apply_rope(jnp.dot(hidden, w_key, preferred_element_type=jnp.float32), cos_t, sin_t).astype(jnp.bfloat16)
    v_new = jnp.dot(hidden, w_value, preferred_element_type=jnp.float32).astype(jnp.bfloat16)
    positions = jnp.arange(SEQ_LEN)
    pos_hit = (positions[None, :] == lengths[:, None])[:, :, None]
    k_all = jnp.where(pos_hit, k_new[:, None, :], k_cache)
    v_all = jnp.where(pos_hit, v_new[:, None, :], v_cache)
    key_valid = positions[None, :] <= lengths[:, None]
    att_scale = HEAD_DIM ** -0.5

    def one_row(row_args):
        q_row, k_row, v_row, valid_row = row_args
        scores = jnp.einsum('hd,sd->hs', q_row.astype(jnp.float32), k_row.astype(jnp.float32)) * att_scale
        scores = jnp.where(valid_row[None, :], scores, -jnp.inf)
        probs_row = jax.nn.softmax(scores, axis=-1)
        return jnp.einsum('hs,sd->hd', probs_row, v_row.astype(jnp.float32))

    attn_out = lax.map(one_row, (q_rot, k_all, v_all, key_valid)).astype(jnp.bfloat16).reshape(BATCH_ROWS, q_cols)
    y_out = jnp.dot(attn_out, w_out, preferred_element_type=jnp.float32).astype(jnp.bfloat16)
    return (y_out, k_new, v_new)
```

```python
import math
import jax
import jax.numpy as jnp
from jax import lax
from jax.experimental import pallas as pl
from jax.experimental.pallas import tpu as pltpu
from jax.sharding import PartitionSpec as P

ROPE_BASE = 10000.0
GROUP = 8
RING = 3
CHUNK = 1024
TAIL_CHUNK = 512
MASKED = -3e38
MESH = pl.DeviceIdType.MESH
Y_BATCHES = {3: (0, 2), 5: (2, 2), 6: (4, 1)}


def make_kernel(rows, embed, seq, heads_local, hd):
    n_groups = rows // GROUP
    n_heads = 4 * heads_local
    assert n_heads * GROUP == hd and hd == 128
    q_cols = heads_local * hd
    last = n_groups - 1
    exp_c = hd ** -0.5 * math.log2(math.e)
    n_tail = seq // TAIL_CHUNK
    half = hd // 2
    freqs = [ROPE_BASE ** (-2.0 * i / hd) for i in range(half)]
    prow = heads_local * GROUP

    def kernel(hid_hbm, wq_hbm, wk_hbm, wv_hbm, wo_hbm, k_hbm, v_hbm, len_hbm,
               y_hbm, kn_hbm, vn_hbm,
               hid, wq, wkv, wo, lens_s, kb, vb, qrec, qmat, qblk, sbuf, oacc, mrow,
               knf, vnf, kn16, vn16, snew, psend, prec, attn, ysend, yrec, yout,
               in_sem, ksem, vsem, tsem, qs_sem, qr_sem, ps_sem, pr_sem, ys_sem, yr_sem, out_sem):
        bx = lax.axis_index('bx')
        me = lax.axis_index('sq')
        chip, core = me // 2, me % 2
        peers = [chip * 2 + (1 - core), (1 - chip) * 2 + core, (1 - chip) * 2 + (1 - core)]
        far_first = (1, 2, 0)
        base = me * seq

        def cp(src, dst, sem):
            return pltpu.make_async_copy(src, dst, sem)

        def k_copy(g):
            return cp(k_hbm.at[pl.ds(g * GROUP, GROUP)], kb.at[g % RING], ksem.at[g % RING])

        def v_copy(g):
            return cp(v_hbm.at[pl.ds(g * GROUP, GROUP)], vb.at[g % RING], vsem.at[g % RING])

        def v_tail(c):
            sl = slice(c * TAIL_CHUNK, (c + 1) * TAIL_CHUNK)
            return cp(v_hbm.at[last * GROUP:rows, sl, :], vb.at[last % RING, :, sl, :], tsem.at[c])

        ins = [cp(len_hbm, lens_s, in_sem.at[0]), cp(hid_hbm, hid, in_sem.at[1]), cp(wq_hbm, wq, in_sem.at[2]),
               cp(wk_hbm, wkv.at[0], in_sem.at[3]), cp(wv_hbm, wkv.at[1], in_sem.at[4]), cp(wo_hbm, wo, in_sem.at[5])]
        for c in ins[:5]:
            c.start()
        k_copy(0).start()
        k_copy(1).start()
        v_copy(0).start()

        barrier = pltpu.get_barrier_semaphore()
        for p in peers:
            pl.semaphore_signal(barrier, inc=1, device_id=(bx, p), device_id_type=MESH)

        k_copy(2).start()
        v_copy(1).start()
        ins[5].start()

        lane = lax.broadcasted_iota(jnp.int32, (1, hd), 1)
        lane_i = lane % half
        freq = jnp.zeros((1, hd), jnp.float32)
        for i in range(half):
            freq = jnp.where(lane_i == i, jnp.float32(freqs[i]), freq)
        ins[0].wait()
        sub = lax.broadcasted_iota(jnp.int32, (GROUP, 1), 0)
        pos_rows = []
        for g in range(n_groups):
            t = jnp.zeros((GROUP, 1), jnp.int32)
            for r in range(GROUP):
                t = jnp.where(sub == r, lens_s[g * GROUP + r], t)
            pos_rows.append(t)
        t_col = jnp.concatenate(pos_rows, axis=0).astype(jnp.float32)
        ang = t_col * freq
        cos_t = jnp.cos(ang)
        sin_t = jnp.where(lane < half, -1.0, 1.0) * jnp.sin(ang)

        def rope(x):
            return x * cos_t + pltpu.roll(x, half, 1) * sin_t

        ins[1].wait()
        ins[2].wait()
        qp = jnp.dot(hid[...], wq[...], preferred_element_type=jnp.float32)
        for h in range(heads_local):
            cs = slice(h * hd, (h + 1) * hd)
            qrec[me, :, cs] = rope(qp[:, cs]).astype(jnp.bfloat16).astype(jnp.float32)
        pl.semaphore_wait(barrier, 3)

        def q_copy(g, d):
            sl = pl.ds(g * GROUP, GROUP)
            return pltpu.make_async_remote_copy(
                src_ref=qrec.at[me, sl], dst_ref=qrec.at[me, sl], send_sem=qs_sem.at[d, g],
                recv_sem=qr_sem.at[d, g], device_id=(bx, peers[d]), device_id_type=MESH)

        for g in range(n_groups):
            for d in far_first:
                q_copy(g, d).start()

        ins[3].wait()
        ins[4].wait()
        kn = rope(jnp.dot(hid[...], wkv[0], preferred_element_type=jnp.float32)).astype(jnp.bfloat16)
        vn = jnp.dot(hid[...], wkv[1], preferred_element_type=jnp.float32).astype(jnp.bfloat16)
        kn16[...] = kn
        vn16[...] = vn
        cp(kn16, kn_hbm, out_sem.at[0]).start()
        cp(vn16, vn_hbm, out_sem.at[1]).start()
        knf = kn.astype(jnp.float32)
        vnf[...] = vn.astype(jnp.float32)
        for h in range(heads_local):
            s_h = jnp.sum(qrec[me, :, h * hd:(h + 1) * hd] * knf, axis=1, keepdims=True)
            snew[h] = jnp.broadcast_to(s_h, (rows, hd))

        lane_r = lane // n_heads

        def lens_row(g):
            out = jnp.zeros((1, hd), jnp.int32)
            for r in range(GROUP):
                out = jnp.where(lane_r == r, lens_s[g * GROUP + r], out)
            return out

        def q_wait(g):
            for d in range(3):
                q_copy(g, d).wait_recv()

        def build_q(g):
            for s in range(4):
                for h in range(heads_local):
                    qmat[pl.ds(s * heads_local + h, GROUP, stride=n_heads), :] = (
                        qrec[s, g * GROUP:(g + 1) * GROUP, h * hd:(h + 1) * hd])
            qt = qmat[...].T.astype(jnp.bfloat16)
            for r in range(GROUP):
                qblk[r * hd:(r + 1) * hd, :] = jnp.where(lane_r == r, qt, jnp.zeros_like(qt))

        def scores(g, c, ln):
            sl = slice(c * CHUNK, (c + 1) * CHUNK)
            kc = jnp.concatenate([kb[g % RING, r, sl, :] for r in range(GROUP)], axis=1)
            s = jnp.dot(kc, qblk[...], preferred_element_type=jnp.float32)
            pos = lax.broadcasted_iota(jnp.int32, (CHUNK, hd), 0) + (base + c * CHUNK)
            s = jnp.where(pos < ln, s, MASKED)
            sbuf[g % 2, sl, :] = s
            return jnp.max(s.reshape(CHUNK // 8, 8, hd), axis=0)

        def values(g, lo, size, mu):
            s = sbuf[g % 2, lo:lo + size, :]
            w = jnp.exp2((s - mu) * exp_c)
            part = jnp.sum(w.reshape(size // 8, 8, hd), axis=0)
            wt = w.astype(jnp.bfloat16).T
            for r in range(GROUP):
                rs = slice(r * n_heads, (r + 1) * n_heads)
                o = jnp.dot(wt[rs, :], vb[g % RING, r, lo:lo + size, :], preferred_element_type=jnp.float32)
                if lo == 0:
                    oacc[rs, :] = o
                else:
                    oacc[rs, :] += o
            return part

        def keep_max(g, m):
            mrow[g % 2] = jnp.broadcast_to(jnp.max(m, axis=0, keepdims=True), (8, hd))

        def p_copy(g, d):
            return pltpu.make_async_remote_copy(
                src_ref=psend.at[g, peers[d]], dst_ref=prec.at[d, g], send_sem=ps_sem.at[d, g],
                recv_sem=pr_sem.at[d, g], device_id=(bx, peers[d]), device_id_type=MESH)

        def send_part(g, l):
            for h in range(n_heads):
                k, hh = h // heads_local, h % heads_local
                psend[g, k, hh * GROUP:(hh + 1) * GROUP, :] = oacc[pl.ds(h, GROUP, stride=n_heads), :]
            l_row = jnp.sum(l, axis=0, keepdims=True)
            ml = jnp.where(sub == 0, mrow[g % 2], jnp.where(sub == 1, l_row, 0.0))
            for k in range(4):
                psend[g, k, prow:prow + 8, :] = ml
            for d in far_first:
                p_copy(g, d).start()

        prow_i = lax.broadcasted_iota(jnp.int32, (prow, hd), 0)
        pick = (prow_i % GROUP) * n_heads + me * heads_local + prow_i // GROUP
        lane_p = lax.broadcasted_iota(jnp.int32, (prow, hd), 1)
        picked = lane_p == pick

        def to_col(row):
            return jnp.sum(jnp.where(picked, row, 0.0), axis=1, keepdims=True)

        def combine(g):
            parts = [psend[g, me]] + [prec[d, g] for d in range(3)]
            rs = slice(g * GROUP, (g + 1) * GROUP)
            s_new = jnp.concatenate([snew[h, rs, :] for h in range(heads_local)], axis=0)
            ms = [to_col(p[prow:prow + 1, :]) for p in parts]
            ls = [to_col(p[prow + 1:prow + 2, :]) for p in parts]
            top = s_new
            for m in ms:
                top = jnp.maximum(top, m)
            f_new = jnp.exp2((s_new - top) * exp_c)
            den = f_new
            v_rows = vnf[rs, :]
            num = f_new * jnp.concatenate([v_rows] * heads_local, axis=0)
            for p, m, l in zip(parts, ms, ls):
                f = jnp.exp2((m - top) * exp_c)
                den = den + f * l
                num = num + f * p[:prow, :]
            o = num / den
            for h in range(heads_local):
                attn[rs, h * hd:(h + 1) * hd] = o[h * GROUP:(h + 1) * GROUP, :]

        def p_wait(g):
            for d in range(3):
                p_copy(g, d).wait_recv()

        y_batches = []

        def y_copy(b, g0, ng, d):
            sl = pl.ds(g0 * GROUP, ng * GROUP)
            return pltpu.make_async_remote_copy(
                src_ref=ysend.at[peers[d], sl], dst_ref=yrec.at[d, sl], send_sem=ys_sem.at[d, b],
                recv_sem=yr_sem.at[d, b], device_id=(bx, peers[d]), device_id_type=MESH)

        def project(g0, ng):
            b = len(y_batches)
            y_batches.append((b, g0, ng))
            sl = slice(g0 * GROUP, (g0 + ng) * GROUP)
            yp = jnp.dot(attn[sl, :].astype(jnp.bfloat16), wo[...], preferred_element_type=jnp.float32)
            for k in range(4):
                ysend[k, sl, :] = yp[:, k * q_cols:(k + 1) * q_cols]
            for d in far_first:
                y_copy(b, g0, ng, d).start()

        def finish(b, g0, ng):
            for d in range(3):
                y_copy(b, g0, ng, d).wait_recv()
            sl = slice(g0 * GROUP, (g0 + ng) * GROUP)
            yout[sl, :] = (ysend[me, sl, :] + yrec[0, sl, :] + yrec[1, sl, :] + yrec[2, sl, :]).astype(jnp.bfloat16)

        q_wait(0)
        build_q(0)
        k_copy(0).wait()
        ln = lens_row(0)
        m = jnp.full((8, hd), MASKED, jnp.float32)
        for c in range(seq // CHUNK):
            m = jnp.maximum(m, scores(0, c, ln))
        keep_max(0, m)

        def shift(g):
            return jnp.where(lens_row(g) > base, mrow[g % 2, 0:1, :], 0.0)

        for g in range(last):
            if g + 3 < n_groups:
                k_copy(g + 3).start()
            if g + 2 < last:
                v_copy(g + 2).start()
            if g + 2 == last:
                for c in range(n_tail):
                    v_tail(c).start()
            q_wait(g + 1)
            if g >= 2:
                p_wait(g - 2)
            if g == 3:
                ins[5].wait()
            k_copy(g + 1).wait()
            v_copy(g).wait()
            build_q(g + 1)
            mu = shift(g)
            ln = lens_row(g + 1)
            m = jnp.full((8, hd), MASKED, jnp.float32)
            l = jnp.zeros((8, hd), jnp.float32)
            for c in range(seq // CHUNK):
                l = l + values(g, c * CHUNK, CHUNK, mu)
                m = jnp.maximum(m, scores(g + 1, c, ln))
            keep_max(g + 1, m)
            send_part(g, l)
            if g >= 2:
                combine(g - 2)
            if g in Y_BATCHES:
                project(*Y_BATCHES[g])

        mu = shift(last)
        l = jnp.zeros((8, hd), jnp.float32)
        for c in range(n_tail):
            v_tail(c).wait()
            l = l + values(last, c * TAIL_CHUNK, TAIL_CHUNK, mu)
        send_part(last, l)
        p_wait(last - 2)
        combine(last - 2)
        p_wait(last - 1)
        combine(last - 1)
        project(last - 2, 2)
        for b in y_batches[:-1]:
            finish(*b)
        p_wait(last)
        combine(last)
        project(last, 1)
        finish(*y_batches[-2])
        finish(*y_batches[-1])
        y_out = cp(yout, y_hbm, out_sem.at[2])
        y_out.start()
        for g in range(n_groups):
            for d in range(3):
                q_copy(g, d).wait_send()
                p_copy(g, d).wait_send()
        for b in y_batches:
            for d in range(3):
                y_copy(*b, d).wait_send()
        cp(kn16, kn_hbm, out_sem.at[0]).wait()
        cp(vn16, vn_hbm, out_sem.at[1]).wait()
        y_out.wait()

    f32, bf16 = jnp.float32, jnp.bfloat16
    dma = pltpu.SemaphoreType.DMA
    n_b = len(Y_BATCHES) + 2
    scratch = [
        pltpu.VMEM((rows, embed), bf16), pltpu.VMEM((embed, q_cols), bf16), pltpu.VMEM((2, embed, hd), bf16),
        pltpu.VMEM((q_cols, embed), bf16), pltpu.SMEM((rows,), jnp.int32),
        pltpu.VMEM((RING, GROUP, seq, hd), bf16), pltpu.VMEM((RING, GROUP, seq, hd), bf16),
        pltpu.VMEM((4, rows, q_cols), f32), pltpu.VMEM((hd, hd), f32), pltpu.VMEM((GROUP * hd, hd), bf16),
        pltpu.VMEM((2, seq, hd), f32), pltpu.VMEM((hd, hd), f32), pltpu.VMEM((2, 8, hd), f32),
        pltpu.VMEM((rows, hd), f32), pltpu.VMEM((rows, hd), f32),
        pltpu.VMEM((rows, hd), bf16), pltpu.VMEM((rows, hd), bf16), pltpu.VMEM((heads_local, rows, hd), f32),
        pltpu.VMEM((n_groups, 4, prow + 8, hd), f32), pltpu.VMEM((3, n_groups, prow + 8, hd), f32),
        pltpu.VMEM((rows, q_cols), f32), pltpu.VMEM((4, rows, q_cols), f32), pltpu.VMEM((3, rows, q_cols), f32),
        pltpu.VMEM((rows, q_cols), bf16),
        dma((6,)), dma((RING,)), dma((RING,)), dma((n_tail,)), dma((3, n_groups)), dma((3, n_groups)),
        dma((3, n_groups)), dma((3, n_groups)), dma((3, n_b)), dma((3, n_b)), dma((3,)),
    ]
    return kernel, scratch


def solution(mesh):
    def local_step(hidden, w_query, w_key, w_value, w_out, k_cache, v_cache, lengths):
        rows, embed = hidden.shape
        hd = w_key.shape[1]
        seq = k_cache.shape[1]
        heads_local = w_query.shape[1] // hd
        q_cols = heads_local * hd
        kernel, scratch = make_kernel(rows, embed, seq, heads_local, hd)
        any_spec = pl.BlockSpec(memory_space=pl.ANY)
        return pl.pallas_call(
            kernel,
            out_shape=(jax.ShapeDtypeStruct((rows, q_cols), jnp.bfloat16),
                       jax.ShapeDtypeStruct((rows, hd), jnp.bfloat16),
                       jax.ShapeDtypeStruct((rows, hd), jnp.bfloat16)),
            in_specs=[any_spec] * 8,
            out_specs=(any_spec,) * 3,
            scratch_shapes=scratch,
            compiler_params=pltpu.CompilerParams(
                collective_id=0, has_side_effects=True, vmem_limit_bytes=67043328),
            name="mqa_decode",
        )(hidden, w_query, w_key, w_value, w_out, k_cache, v_cache, lengths)

    return jax.shard_map(
        local_step,
        mesh=mesh,
        in_specs=(P('bx', None), P(None, 'sq'), P(None, None), P(None, None), P('sq', None),
                  P('bx', 'sq', None), P('bx', 'sq', None), P('bx')),
        out_specs=(P('bx', 'sq'), P('bx', None), P('bx', None)),
        check_vma=False,
    )
```

```python
import math
import jax
import jax.numpy as jnp
from jax import lax
from jax.experimental import pallas as pl
from jax.experimental.pallas import tpu as pltpu
from jax.sharding import PartitionSpec as P

ROPE_BASE = 10000.0
GROUP = 8
RING = 3
CHUNK = 1024
TAIL_CHUNK = 512
MASKED = -3e38
MESH = pl.DeviceIdType.MESH
Y_BATCHES = {3: (0, 2), 5: (2, 2), 6: (4, 1)}


def make_kernel(rows, embed, seq, heads_local, hd):
    n_groups = rows // GROUP
    n_heads = 4 * heads_local
    assert n_heads * GROUP == hd and hd == 128
    q_cols = heads_local * hd
    last = n_groups - 1
    exp_c = hd ** -0.5 * math.log2(math.e)
    n_tail = seq // TAIL_CHUNK
    half = hd // 2
    freqs = [ROPE_BASE ** (-2.0 * i / hd) for i in range(half)]
    prow = heads_local * GROUP

    def kernel(hid_hbm, wq_hbm, wk_hbm, wv_hbm, wo_hbm, k_hbm, v_hbm, len_hbm,
               y_hbm, kn_hbm, vn_hbm,
               hid, wq, wkv, wo, lens_s, kb, vb, qown, qrec, qmat, qblk, sbuf, oacc, mrow,
               vnf, kn16, vn16, snew, psend, prec, attn, ysend, yrec, yout,
               in_sem, ksem, vsem, tsem, qs_sem, qr_sem, ps_sem, pr_sem, ys_sem, yr_sem, out_sem):
        bx = lax.axis_index('bx')
        me = lax.axis_index('sq')
        chip, core = me // 2, me % 2
        peers = [chip * 2 + (1 - core), (1 - chip) * 2 + core, (1 - chip) * 2 + (1 - core)]
        far_first = (1, 2, 0)
        base = me * seq

        def cp(src, dst, sem):
            return pltpu.make_async_copy(src, dst, sem)

        def k_copy(g):
            return cp(k_hbm.at[pl.ds(g * GROUP, GROUP)], kb.at[g % RING], ksem.at[g % RING])

        def v_copy(g):
            return cp(v_hbm.at[pl.ds(g * GROUP, GROUP)], vb.at[g % RING], vsem.at[g % RING])

        def v_tail(c):
            sl = slice(c * TAIL_CHUNK, (c + 1) * TAIL_CHUNK)
            return cp(v_hbm.at[last * GROUP:rows, sl, :], vb.at[last % RING, :, sl, :], tsem.at[c])

        ins = [cp(len_hbm, lens_s, in_sem.at[0]), cp(hid_hbm, hid, in_sem.at[1]), cp(wq_hbm, wq, in_sem.at[2]),
               cp(wk_hbm, wkv.at[0], in_sem.at[3]), cp(wv_hbm, wkv.at[1], in_sem.at[4]), cp(wo_hbm, wo, in_sem.at[5])]
        for c in ins[:5]:
            c.start()
        k_copy(0).start()
        k_copy(1).start()
        v_copy(0).start()

        barrier = pltpu.get_barrier_semaphore()
        for p in peers:
            pl.semaphore_signal(barrier, inc=1, device_id=(bx, p), device_id_type=MESH)

        k_copy(2).start()
        v_copy(1).start()
        ins[5].start()

        lane = lax.broadcasted_iota(jnp.int32, (1, hd), 1)
        lane_i = lane % half
        freq = jnp.zeros((1, hd), jnp.float32)
        for i in range(half):
            freq = jnp.where(lane_i == i, jnp.float32(freqs[i]), freq)
        ins[0].wait()
        sub = lax.broadcasted_iota(jnp.int32, (GROUP, 1), 0)
        pos_rows = []
        for g in range(n_groups):
            t = jnp.zeros((GROUP, 1), jnp.int32)
            for r in range(GROUP):
                t = jnp.where(sub == r, lens_s[g * GROUP + r], t)
            pos_rows.append(t)
        t_col = jnp.concatenate(pos_rows, axis=0).astype(jnp.float32)
        ang = t_col * freq
        cos_t = jnp.cos(ang)
        sin_t = jnp.where(lane < half, -1.0, 1.0) * jnp.sin(ang)

        def rope(x):
            return x * cos_t + pltpu.roll(x, half, 1) * sin_t

        ins[1].wait()
        ins[2].wait()
        qp = jnp.dot(hid[...], wq[...], preferred_element_type=jnp.float32)
        for h in range(heads_local):
            cs = slice(h * hd, (h + 1) * hd)
            q_h = rope(qp[:, cs]).astype(jnp.bfloat16).astype(jnp.float32)
            qown[:, :, cs] = q_h.reshape(n_groups, GROUP, hd)
        pl.semaphore_wait(barrier, 3)

        def q_copy(g, d):
            return pltpu.make_async_remote_copy(
                src_ref=qown.at[g], dst_ref=qrec.at[g, d], send_sem=qs_sem.at[d],
                recv_sem=qr_sem.at[g], device_id=(bx, peers[d]), device_id_type=MESH)

        for g in range(n_groups):
            for d in far_first:
                q_copy(g, d).start()

        ins[3].wait()
        ins[4].wait()
        kn = rope(jnp.dot(hid[...], wkv[0], preferred_element_type=jnp.float32)).astype(jnp.bfloat16)
        vn = jnp.dot(hid[...], wkv[1], preferred_element_type=jnp.float32).astype(jnp.bfloat16)
        kn16[...] = kn
        vn16[...] = vn
        cp(kn16, kn_hbm, out_sem.at[0]).start()
        cp(vn16, vn_hbm, out_sem.at[1]).start()
        knf = kn.astype(jnp.float32)
        vnf[...] = vn.astype(jnp.float32)
        for h in range(heads_local):
            q_h = qown[:, :, h * hd:(h + 1) * hd].reshape(rows, hd)
            s_h = jnp.sum(q_h * knf, axis=1, keepdims=True)
            snew[h] = jnp.broadcast_to(s_h, (rows, hd))

        lane_r = lane // n_heads

        def lens_row(g):
            out = jnp.zeros((1, hd), jnp.int32)
            for r in range(GROUP):
                out = jnp.where(lane_r == r, lens_s[g * GROUP + r], out)
            return out

        def q_wait(g):
            pltpu.make_async_copy(qrec.at[g], qrec.at[g], qr_sem.at[g]).wait()

        def build_q(g):
            for s in range(4):
                for h in range(heads_local):
                    cs = slice(h * hd, (h + 1) * hd)
                    blk = qown[g, :, cs] if s == 3 else qrec[g, s, :, cs]
                    qmat[pl.ds(s * heads_local + h, GROUP, stride=n_heads), :] = blk
            qt = qmat[...].T.astype(jnp.bfloat16)
            for r in range(GROUP):
                qblk[r * hd:(r + 1) * hd, :] = jnp.where(lane_r == r, qt, jnp.zeros_like(qt))

        def scores(g, c, ln):
            sl = slice(c * CHUNK, (c + 1) * CHUNK)
            kc = jnp.concatenate([kb[g % RING, r, sl, :] for r in range(GROUP)], axis=1)
            s = jnp.dot(kc, qblk[...], preferred_element_type=jnp.float32)
            pos = lax.broadcasted_iota(jnp.int32, (CHUNK, hd), 0) + (base + c * CHUNK)
            s = jnp.where(pos < ln, s, MASKED)
            sbuf[g % 2, sl, :] = s
            return jnp.max(s.reshape(CHUNK // 8, 8, hd), axis=0)

        def values(g, lo, size, mu):
            s = sbuf[g % 2, lo:lo + size, :]
            w = jnp.exp2((s - mu) * exp_c)
            part = jnp.sum(w.reshape(size // 8, 8, hd), axis=0)
            wt = w.astype(jnp.bfloat16).T
            for r in range(0, GROUP, 2):
                rs = slice(r * n_heads, (r + 2) * n_heads)
                vc = jnp.concatenate([vb[g % RING, r + i, lo:lo + size, :] for i in range(2)], axis=1)
                o = jnp.dot(wt[rs, :], vc, preferred_element_type=jnp.float32)
                o = jnp.concatenate([o[:n_heads, :hd], o[n_heads:, hd:]], axis=0)
                if lo == 0:
                    oacc[rs, :] = o
                else:
                    oacc[rs, :] += o
            return part

        def keep_max(g, m):
            mrow[g % 2] = jnp.broadcast_to(jnp.max(m, axis=0, keepdims=True), (8, hd))

        def p_copy(g, d):
            return pltpu.make_async_remote_copy(
                src_ref=psend.at[d, g], dst_ref=prec.at[g, d], send_sem=ps_sem.at[d],
                recv_sem=pr_sem.at[g], device_id=(bx, peers[d]), device_id_type=MESH)

        def send_part(g, l):
            for h in range(n_heads):
                k, hh = h // heads_local, h % heads_local
                psend[k, g, hh * GROUP:(hh + 1) * GROUP, :] = oacc[pl.ds(h, GROUP, stride=n_heads), :]
            l_row = jnp.sum(l, axis=0, keepdims=True)
            ml = jnp.where(sub == 0, mrow[g % 2], jnp.where(sub == 1, l_row, 0.0))
            for k in range(4):
                psend[k, g, prow:prow + 8, :] = ml
            for d in far_first:
                p_copy(g, d).start()

        prow_i = lax.broadcasted_iota(jnp.int32, (prow, hd), 0)
        pick = (prow_i % GROUP) * n_heads + prow_i // GROUP
        lane_p = lax.broadcasted_iota(jnp.int32, (prow, hd), 1)
        picked = [lane_p == pick + d * heads_local for d in range(4)]

        def to_col(d, row):
            return jnp.sum(jnp.where(picked[d], row, 0.0), axis=1, keepdims=True)

        def combine(g):
            parts = [prec[g, d] for d in range(3)] + [psend[3, g]]
            rs = slice(g * GROUP, (g + 1) * GROUP)
            s_new = jnp.concatenate([snew[h, rs, :] for h in range(heads_local)], axis=0)
            ms = [to_col(d, p[prow:prow + 1, :]) for d, p in enumerate(parts)]
            ls = [to_col(d, p[prow + 1:prow + 2, :]) for d, p in enumerate(parts)]
            top = s_new
            for m in ms:
                top = jnp.maximum(top, m)
            f_new = jnp.exp2((s_new - top) * exp_c)
            den = f_new
            v_rows = vnf[rs, :]
            num = f_new * jnp.concatenate([v_rows] * heads_local, axis=0)
            for p, m, l in zip(parts, ms, ls):
                f = jnp.exp2((m - top) * exp_c)
                den = den + f * l
                num = num + f * p[:prow, :]
            o = num / den
            for h in range(heads_local):
                attn[rs, h * hd:(h + 1) * hd] = o[h * GROUP:(h + 1) * GROUP, :]

        def p_wait(g):
            pltpu.make_async_copy(prec.at[g], prec.at[g], pr_sem.at[g]).wait()

        y_batches = []

        def y_copy(b, g0, ng, d):
            sl = pl.ds(g0 * GROUP, ng * GROUP)
            return pltpu.make_async_remote_copy(
                src_ref=ysend.at[peers[d], sl], dst_ref=yrec.at[d, sl], send_sem=ys_sem.at[d],
                recv_sem=yr_sem.at[b], device_id=(bx, peers[d]), device_id_type=MESH)

        def project(g0, ng):
            b = len(y_batches)
            y_batches.append((b, g0, ng))
            sl = slice(g0 * GROUP, (g0 + ng) * GROUP)
            yp = jnp.dot(attn[sl, :].astype(jnp.bfloat16), wo[...], preferred_element_type=jnp.float32)
            for k in range(4):
                ysend[k, sl, :] = yp[:, k * q_cols:(k + 1) * q_cols]
            for d in far_first:
                y_copy(b, g0, ng, d).start()

        def finish(b, g0, ng):
            sl = slice(g0 * GROUP, (g0 + ng) * GROUP)
            pltpu.make_async_copy(yrec.at[:, sl], yrec.at[:, sl], yr_sem.at[b]).wait()
            yout[sl, :] = (ysend[me, sl, :] + yrec[0, sl, :] + yrec[1, sl, :] + yrec[2, sl, :]).astype(jnp.bfloat16)

        q_wait(0)
        build_q(0)
        k_copy(0).wait()
        ln = lens_row(0)
        m = jnp.full((8, hd), MASKED, jnp.float32)
        for c in range(seq // CHUNK):
            m = jnp.maximum(m, scores(0, c, ln))
        keep_max(0, m)

        def shift(g):
            return jnp.where(lens_row(g) > base, mrow[g % 2, 0:1, :], 0.0)

        for g in range(last):
            if g + 3 < n_groups:
                k_copy(g + 3).start()
            if g + 2 < last:
                v_copy(g + 2).start()
            if g + 2 == last:
                for c in range(n_tail):
                    v_tail(c).start()
            q_wait(g + 1)
            if g >= 2:
                p_wait(g - 2)
            if g == 3:
                ins[5].wait()
            k_copy(g + 1).wait()
            v_copy(g).wait()
            build_q(g + 1)
            mu = shift(g)
            ln = lens_row(g + 1)
            m = jnp.full((8, hd), MASKED, jnp.float32)
            l = jnp.zeros((8, hd), jnp.float32)
            for c in range(seq // CHUNK):
                l = l + values(g, c * CHUNK, CHUNK, mu)
                m = jnp.maximum(m, scores(g + 1, c, ln))
            keep_max(g + 1, m)
            send_part(g, l)
            if g >= 2:
                combine(g - 2)
            if g in Y_BATCHES:
                project(*Y_BATCHES[g])

        mu = shift(last)
        l = jnp.zeros((8, hd), jnp.float32)
        for c in range(n_tail):
            v_tail(c).wait()
            l = l + values(last, c * TAIL_CHUNK, TAIL_CHUNK, mu)
        send_part(last, l)
        p_wait(last - 2)
        combine(last - 2)
        p_wait(last - 1)
        combine(last - 1)
        project(last - 2, 2)
        for b in y_batches[:-1]:
            finish(*b)
        p_wait(last)
        combine(last)
        project(last, 1)
        finish(*y_batches[-2])
        finish(*y_batches[-1])
        y_out = cp(yout, y_hbm, out_sem.at[2])
        y_out.start()
        for d in range(3):
            pltpu.make_async_copy(qown, qown, qs_sem.at[d]).wait()
            pltpu.make_async_copy(psend.at[d], psend.at[d], ps_sem.at[d]).wait()
            pltpu.make_async_copy(ysend.at[d], ysend.at[d], ys_sem.at[d]).wait()
        cp(kn16, kn_hbm, out_sem.at[0]).wait()
        cp(vn16, vn_hbm, out_sem.at[1]).wait()
        y_out.wait()

    f32, bf16 = jnp.float32, jnp.bfloat16
    dma = pltpu.SemaphoreType.DMA
    n_b = len(Y_BATCHES) + 2
    scratch = [
        pltpu.VMEM((rows, embed), bf16), pltpu.VMEM((embed, q_cols), bf16), pltpu.VMEM((2, embed, hd), bf16),
        pltpu.VMEM((q_cols, embed), bf16), pltpu.SMEM((rows,), jnp.int32),
        pltpu.VMEM((RING, GROUP, seq, hd), bf16), pltpu.VMEM((RING, GROUP, seq, hd), bf16),
        pltpu.VMEM((n_groups, GROUP, q_cols), f32), pltpu.VMEM((n_groups, 3, GROUP, q_cols), f32),
        pltpu.VMEM((hd, hd), f32), pltpu.VMEM((GROUP * hd, hd), bf16),
        pltpu.VMEM((2, seq, hd), f32), pltpu.VMEM((hd, hd), f32), pltpu.VMEM((2, 8, hd), f32),
        pltpu.VMEM((rows, hd), f32),
        pltpu.VMEM((rows, hd), bf16), pltpu.VMEM((rows, hd), bf16), pltpu.VMEM((heads_local, rows, hd), f32),
        pltpu.VMEM((4, n_groups, prow + 8, hd), f32), pltpu.VMEM((n_groups, 3, prow + 8, hd), f32),
        pltpu.VMEM((rows, q_cols), f32), pltpu.VMEM((4, rows, q_cols), f32), pltpu.VMEM((3, rows, q_cols), f32),
        pltpu.VMEM((rows, q_cols), bf16),
        dma((6,)), dma((RING,)), dma((RING,)), dma((n_tail,)), dma((3,)), dma((n_groups,)),
        dma((3,)), dma((n_groups,)), dma((3,)), dma((n_b,)), dma((3,)),
    ]
    return kernel, scratch


def store_kernel(y_ref, k_ref, v_ref, yo_ref, ko_ref, vo_ref, y_buf, k_buf, v_buf, sem):
    trips = [(y_ref, y_buf, yo_ref), (k_ref, k_buf, ko_ref), (v_ref, v_buf, vo_ref)]
    reads = [pltpu.make_async_copy(a, b, sem.at[i]) for i, (a, b, _) in enumerate(trips)]
    writes = [pltpu.make_async_copy(b, c, sem.at[3 + i]) for i, (_, b, c) in enumerate(trips)]
    for c in reads:
        c.start()
    for r, w in zip(reads, writes):
        r.wait()
        w.start()
    for w in writes:
        w.wait()


def solution(mesh):
    def local_step(hidden, w_query, w_key, w_value, w_out, k_cache, v_cache, lengths):
        rows, embed = hidden.shape
        hd = w_key.shape[1]
        seq = k_cache.shape[1]
        heads_local = w_query.shape[1] // hd
        q_cols = heads_local * hd
        kernel, scratch = make_kernel(rows, embed, seq, heads_local, hd)
        any_spec = pl.BlockSpec(memory_space=pl.ANY)
        outs = (jax.ShapeDtypeStruct((rows, q_cols), jnp.bfloat16),
                jax.ShapeDtypeStruct((rows, hd), jnp.bfloat16),
                jax.ShapeDtypeStruct((rows, hd), jnp.bfloat16))
        raw = pl.pallas_call(
            kernel,
            out_shape=outs,
            in_specs=[any_spec] * 8,
            out_specs=(any_spec,) * 3,
            scratch_shapes=scratch,
            compiler_params=pltpu.CompilerParams(
                collective_id=0, has_side_effects=True, vmem_limit_bytes=67043328),
            name="mqa_decode",
        )(hidden, w_query, w_key, w_value, w_out, k_cache, v_cache, lengths)
        return pl.pallas_call(
            store_kernel,
            out_shape=outs,
            in_specs=[any_spec] * 3,
            out_specs=(any_spec,) * 3,
            scratch_shapes=[pltpu.VMEM(o.shape, o.dtype) for o in outs] + [pltpu.SemaphoreType.DMA((6,))],
            name="store_outputs",
        )(*raw)

    return jax.shard_map(
        local_step,
        mesh=mesh,
        in_specs=(P('bx', None), P(None, 'sq'), P(None, None), P(None, None), P('sq', None),
                  P('bx', 'sq', None), P('bx', 'sq', None), P('bx')),
        out_specs=(P('bx', 'sq'), P('bx', None), P('bx', None)),
        check_vma=False,
    )
```

```python
import math
import jax
import jax.numpy as jnp
from jax import lax
from jax.experimental import pallas as pl
from jax.experimental.pallas import tpu as pltpu
from jax.sharding import PartitionSpec as P

ROPE_BASE = 10000.0
GROUP = 8
RING = 3
CHUNK = 1024
PIECE = 4
MASKED = -3e38
MESH = pl.DeviceIdType.MESH
Y_BATCHES = {3: (0, 2), 5: (2, 2)}


def make_kernel(rows, embed, seq, heads_local, hd):
    n_groups = rows // GROUP
    n_heads = 4 * heads_local
    assert n_heads * GROUP == hd and hd == 128
    q_cols = heads_local * hd
    last = n_groups - 1
    exp_c = hd ** -0.5 * math.log2(math.e)
    n_pieces = GROUP // PIECE
    piece_rows = heads_local * PIECE
    half = hd // 2
    freqs = [ROPE_BASE ** (-2.0 * i / hd) for i in range(half)]
    prow = heads_local * GROUP

    def kernel(hid_hbm, wq_hbm, wk_hbm, wv_hbm, wo_hbm, k_hbm, v_hbm, len_hbm,
               y_hbm, kn_hbm, vn_hbm,
               hid, wq, wkv, wo, lens_s, kb, vb, qown, qrec, qmat, qblk, sbuf, oacc, mrow,
               vnf, kn16, vn16, snew, wts, psend, prec, tsend, trec, attn, ysend,
               in_sem, ksem, vsem, tsem, qs_sem, qr_sem, ps_sem, pr_sem, ts_sem, tr_sem, ys_sem, yr_sem,
               out_sem):
        bx = lax.axis_index('bx')
        me = lax.axis_index('sq')
        chip, core = me // 2, me % 2
        peers = [chip * 2 + (1 - core), (1 - chip) * 2 + core, (1 - chip) * 2 + (1 - core)]
        far_first = (1, 2, 0)
        base = me * seq

        def cp(src, dst, sem):
            return pltpu.make_async_copy(src, dst, sem)

        def k_copy(g):
            return cp(k_hbm.at[pl.ds(g * GROUP, GROUP)], kb.at[g % RING], ksem.at[g % RING])

        def v_copy(g):
            return cp(v_hbm.at[pl.ds(g * GROUP, GROUP)], vb.at[g % RING], vsem.at[g % RING])

        def v_tail(c):
            r0 = last * GROUP + c * PIECE
            return cp(v_hbm.at[r0:r0 + PIECE], vb.at[last % RING, c * PIECE:(c + 1) * PIECE], tsem.at[c])

        ins = [cp(len_hbm, lens_s, in_sem.at[0]), cp(hid_hbm, hid, in_sem.at[1]), cp(wq_hbm, wq, in_sem.at[2]),
               cp(wk_hbm, wkv.at[0], in_sem.at[3]), cp(wv_hbm, wkv.at[1], in_sem.at[4]), cp(wo_hbm, wo, in_sem.at[5])]
        for c in ins[:5]:
            c.start()
        k_copy(0).start()
        k_copy(1).start()
        v_copy(0).start()

        barrier = pltpu.get_barrier_semaphore()
        for p in peers:
            pl.semaphore_signal(barrier, inc=1, device_id=(bx, p), device_id_type=MESH)

        k_copy(2).start()
        v_copy(1).start()
        ins[5].start()

        lane = lax.broadcasted_iota(jnp.int32, (1, hd), 1)
        lane_i = lane % half
        freq = jnp.zeros((1, hd), jnp.float32)
        for i in range(half):
            freq = jnp.where(lane_i == i, jnp.float32(freqs[i]), freq)
        ins[0].wait()
        sub = lax.broadcasted_iota(jnp.int32, (GROUP, 1), 0)
        pos_rows = []
        for g in range(n_groups):
            t = jnp.zeros((GROUP, 1), jnp.int32)
            for r in range(GROUP):
                t = jnp.where(sub == r, lens_s[g * GROUP + r], t)
            pos_rows.append(t)
        t_col = jnp.concatenate(pos_rows, axis=0).astype(jnp.float32)
        ang = t_col * freq
        cos_t = jnp.cos(ang)
        sin_t = jnp.where(lane < half, -1.0, 1.0) * jnp.sin(ang)

        def rope(x):
            return x * cos_t + pltpu.roll(x, half, 1) * sin_t

        ins[1].wait()
        ins[2].wait()
        qp = jnp.dot(hid[...], wq[...], preferred_element_type=jnp.float32)
        for h in range(heads_local):
            cs = slice(h * hd, (h + 1) * hd)
            q_h = rope(qp[:, cs]).astype(jnp.bfloat16).astype(jnp.float32)
            qown[:, :, cs] = q_h.reshape(n_groups, GROUP, hd)
        pl.semaphore_wait(barrier, 3)

        def q_copy(g, d):
            return pltpu.make_async_remote_copy(
                src_ref=qown.at[g], dst_ref=qrec.at[g, d], send_sem=qs_sem.at[d],
                recv_sem=qr_sem.at[g], device_id=(bx, peers[d]), device_id_type=MESH)

        for g in range(n_groups):
            for d in far_first:
                q_copy(g, d).start()

        ins[3].wait()
        ins[4].wait()
        kn = rope(jnp.dot(hid[...], wkv[0], preferred_element_type=jnp.float32)).astype(jnp.bfloat16)
        vn = jnp.dot(hid[...], wkv[1], preferred_element_type=jnp.float32).astype(jnp.bfloat16)
        kn16[...] = kn
        vn16[...] = vn
        cp(kn16, kn_hbm, out_sem.at[0]).start()
        cp(vn16, vn_hbm, out_sem.at[1]).start()
        knf = kn.astype(jnp.float32)
        vnf[...] = vn.astype(jnp.float32)
        for h in range(heads_local):
            q_h = qown[:, :, h * hd:(h + 1) * hd].reshape(rows, hd)
            s_h = jnp.sum(q_h * knf, axis=1, keepdims=True)
            snew[h] = jnp.broadcast_to(s_h, (rows, hd))

        lane_r = lane // n_heads

        def lens_row(g):
            out = jnp.zeros((1, hd), jnp.int32)
            for r in range(GROUP):
                out = jnp.where(lane_r == r, lens_s[g * GROUP + r], out)
            return out

        def q_wait(g):
            pltpu.make_async_copy(qrec.at[g], qrec.at[g], qr_sem.at[g]).wait()

        def build_q(g):
            for s in range(4):
                for h in range(heads_local):
                    cs = slice(h * hd, (h + 1) * hd)
                    blk = qown[g, :, cs] if s == 3 else qrec[g, s, :, cs]
                    qmat[pl.ds(s * heads_local + h, GROUP, stride=n_heads), :] = blk
            qt = qmat[...].T.astype(jnp.bfloat16)
            for r in range(GROUP):
                qblk[r * hd:(r + 1) * hd, :] = jnp.where(lane_r == r, qt, jnp.zeros_like(qt))

        def scores(g, c, ln):
            sl = slice(c * CHUNK, (c + 1) * CHUNK)
            kc = jnp.concatenate([kb[g % RING, r, sl, :] for r in range(GROUP)], axis=1)
            s = jnp.dot(kc, qblk[...], preferred_element_type=jnp.float32)
            pos = lax.broadcasted_iota(jnp.int32, (CHUNK, hd), 0) + (base + c * CHUNK)
            s = jnp.where(pos < ln, s, MASKED)
            sbuf[g % 2, sl, :] = s
            return jnp.max(s.reshape(CHUNK // 8, 8, hd), axis=0)

        def weights(g, lo, size, mu):
            w = jnp.exp2((sbuf[g % 2, lo:lo + size, :] - mu) * exp_c)
            part = jnp.sum(w.reshape(size // 8, 8, hd), axis=0)
            return w.astype(jnp.bfloat16).T, part

        def weighted(g, r, wt, lo, size):
            vc = jnp.concatenate([vb[g % RING, r + i, lo:lo + size, :] for i in range(2)], axis=1)
            o = jnp.dot(wt, vc, preferred_element_type=jnp.float32)
            return jnp.concatenate([o[:n_heads, :hd], o[n_heads:, hd:]], axis=0)

        def values(g, lo, size, mu):
            wt, part = weights(g, lo, size, mu)
            for r in range(0, GROUP, 2):
                rs = slice(r * n_heads, (r + 2) * n_heads)
                o = weighted(g, r, wt[rs, :], lo, size)
                if lo == 0:
                    oacc[rs, :] = o
                else:
                    oacc[rs, :] += o
            return part

        def keep_max(g, m):
            mrow[g % 2] = jnp.broadcast_to(jnp.max(m, axis=0, keepdims=True), (8, hd))

        def p_copy(g, d):
            return pltpu.make_async_remote_copy(
                src_ref=psend.at[d, g], dst_ref=prec.at[g, d], send_sem=ps_sem.at[d],
                recv_sem=pr_sem.at[g], device_id=(bx, peers[d]), device_id_type=MESH)

        def send_part(g, l):
            for h in range(n_heads):
                k, hh = h // heads_local, h % heads_local
                psend[k, g, hh * GROUP:(hh + 1) * GROUP, :] = oacc[pl.ds(h, GROUP, stride=n_heads), :]
            l_row = jnp.sum(l, axis=0, keepdims=True)
            ml = jnp.where(sub == 0, mrow[g % 2], jnp.where(sub == 1, l_row, 0.0))
            for k in range(4):
                psend[k, g, prow:prow + 8, :] = ml
            for d in far_first:
                p_copy(g, d).start()

        def t_copy(c, d):
            return pltpu.make_async_remote_copy(
                src_ref=tsend.at[d, c], dst_ref=trec.at[c, d], send_sem=ts_sem.at[d],
                recv_sem=tr_sem.at[c], device_id=(bx, peers[d]), device_id_type=MESH)

        def send_piece(c, l_row):
            ml = jnp.where(sub == 0, mrow[last % 2], jnp.where(sub == 1, l_row, 0.0))
            for h in range(n_heads):
                k, hh = h // heads_local, h % heads_local
                tsend[k, c, hh * PIECE:(hh + 1) * PIECE, :] = (
                    oacc[pl.ds(c * PIECE * n_heads + h, PIECE, stride=n_heads), :])
            for k in range(4):
                tsend[k, c, piece_rows:piece_rows + 8, :] = ml
            for d in far_first:
                t_copy(c, d).start()

        def picks(nr, r0):
            row = lax.broadcasted_iota(jnp.int32, (heads_local * nr, hd), 0)
            at = (r0 + row % nr) * n_heads + row // nr
            lane_p = lax.broadcasted_iota(jnp.int32, (heads_local * nr, hd), 1)
            return [lane_p == at + d * heads_local for d in range(4)]

        def combine_rows(parts, row0, nr, picked):
            n = heads_local * nr
            rs = slice(row0, row0 + nr)

            def to_col(d, row):
                return jnp.sum(jnp.where(picked[d], row, 0.0), axis=1, keepdims=True)

            s_new = jnp.concatenate([snew[h, rs, :] for h in range(heads_local)], axis=0)
            ms = [to_col(d, p[n:n + 1, :]) for d, p in enumerate(parts)]
            ls = [to_col(d, p[n + 1:n + 2, :]) for d, p in enumerate(parts)]
            top = s_new
            for m in ms:
                top = jnp.maximum(top, m)
            f_new = jnp.exp2((s_new - top) * exp_c)
            den = f_new
            num = f_new * jnp.concatenate([vnf[rs, :]] * heads_local, axis=0)
            for p, m, l in zip(parts, ms, ls):
                f = jnp.exp2((m - top) * exp_c)
                den = den + f * l
                num = num + f * p[:n, :]
            o = num / den
            for h in range(heads_local):
                attn[rs, h * hd:(h + 1) * hd] = o[h * nr:(h + 1) * nr, :]

        def combine(g):
            parts = [prec[g, d] for d in range(3)] + [psend[3, g]]
            combine_rows(parts, g * GROUP, GROUP, picks(GROUP, 0))

        def combine_piece(c):
            pltpu.make_async_copy(trec.at[c], trec.at[c], tr_sem.at[c]).wait()
            parts = [trec[c, d] for d in range(3)] + [tsend[3, c]]
            combine_rows(parts, last * GROUP + c * PIECE, PIECE, picks(PIECE, c * PIECE))

        def p_wait(g):
            pltpu.make_async_copy(prec.at[g], prec.at[g], pr_sem.at[g]).wait()

        y_batches = []

        def y_copy(b, g0, ng, d):
            sl = pl.ds(g0 * GROUP, ng * GROUP)
            return pltpu.make_async_remote_copy(
                src_ref=ysend.at[d, sl], dst_ref=y_hbm.at[d, sl], send_sem=ys_sem.at[d],
                recv_sem=yr_sem.at[b], device_id=(bx, peers[d]), device_id_type=MESH)

        def project(g0, ng):
            b = len(y_batches)
            y_batches.append((b, g0, ng))
            sl = slice(g0 * GROUP, (g0 + ng) * GROUP)
            lhs = attn[sl, :].astype(jnp.bfloat16)
            for d in far_first + (3,):
                col = pl.multiple_of((me if d == 3 else peers[d]) * q_cols, q_cols)
                ysend[d, sl, :] = jnp.dot(lhs, wo[:, pl.ds(col, q_cols)], preferred_element_type=jnp.float32)
                if d < 3:
                    y_copy(b, g0, ng, d).start()
                else:
                    cp(ysend.at[3, sl], y_hbm.at[3, sl], out_sem.at[2]).start()

        def finish(b, g0, ng):
            sl = pl.ds(g0 * GROUP, ng * GROUP)
            pltpu.make_async_copy(y_hbm.at[0:3, sl], y_hbm.at[0:3, sl], yr_sem.at[b]).wait()

        q_wait(0)
        build_q(0)
        k_copy(0).wait()
        ln = lens_row(0)
        m = jnp.full((8, hd), MASKED, jnp.float32)
        for c in range(seq // CHUNK):
            m = jnp.maximum(m, scores(0, c, ln))
        keep_max(0, m)

        def shift(g):
            return jnp.where(lens_row(g) > base, mrow[g % 2, 0:1, :], 0.0)

        for g in range(last - 1):
            if g + 3 < n_groups:
                k_copy(g + 3).start()
            if g + 2 < last:
                v_copy(g + 2).start()
            if g + 2 == last:
                for c in range(n_pieces):
                    v_tail(c).start()
            q_wait(g + 1)
            if g >= 2:
                p_wait(g - 2)
            if g == 3:
                ins[5].wait()
            k_copy(g + 1).wait()
            v_copy(g).wait()
            build_q(g + 1)
            mu = shift(g)
            ln = lens_row(g + 1)
            m = jnp.full((8, hd), MASKED, jnp.float32)
            l = jnp.zeros((8, hd), jnp.float32)
            for c in range(seq // CHUNK):
                l = l + values(g, c * CHUNK, CHUNK, mu)
                m = jnp.maximum(m, scores(g + 1, c, ln))
            keep_max(g + 1, m)
            send_part(g, l)
            if g >= 2:
                combine(g - 2)
            if g in Y_BATCHES:
                project(*Y_BATCHES[g])

        pre = last - 1
        q_wait(last)
        p_wait(pre - 2)
        k_copy(last).wait()
        build_q(last)
        ln = lens_row(last)
        m = jnp.full((8, hd), MASKED, jnp.float32)
        for c in range(seq // CHUNK):
            m = jnp.maximum(m, scores(last, c, ln))
        keep_max(last, m)
        combine(pre - 2)
        mu = shift(pre)
        v_copy(pre).wait()
        l = jnp.zeros((8, hd), jnp.float32)
        for c in range(seq // CHUNK):
            l = l + values(pre, c * CHUNK, CHUNK, mu)
        send_part(pre, l)
        mu = shift(last)
        l = jnp.zeros((8, hd), jnp.float32)
        for c in range(seq // CHUNK):
            wt, part = weights(last, c * CHUNK, CHUNK, mu)
            wts[:, c * CHUNK:(c + 1) * CHUNK] = wt
            l = l + part
        l_row = jnp.sum(l, axis=0, keepdims=True)
        for c in range(n_pieces):
            v_tail(c).wait()
            for r in range(c * PIECE, (c + 1) * PIECE, 2):
                rs = slice(r * n_heads, (r + 2) * n_heads)
                oacc[rs, :] = weighted(last, r, wts[rs, :], 0, seq)
            send_piece(c, l_row)
        p_wait(pre - 1)
        combine(pre - 1)
        project(pre - 2, 2)
        p_wait(pre)
        combine(pre)
        project(pre, 1)
        for c in range(n_pieces):
            combine_piece(c)
        project(last, 1)
        for b in y_batches:
            finish(*b)
        for d in range(3):
            pltpu.make_async_copy(qown, qown, qs_sem.at[d]).wait()
            pltpu.make_async_copy(psend.at[d], psend.at[d], ps_sem.at[d]).wait()
            pltpu.make_async_copy(tsend.at[d], tsend.at[d], ts_sem.at[d]).wait()
            pltpu.make_async_copy(ysend.at[d], ysend.at[d], ys_sem.at[d]).wait()
        cp(kn16, kn_hbm, out_sem.at[0]).wait()
        cp(vn16, vn_hbm, out_sem.at[1]).wait()
        cp(ysend.at[3], y_hbm.at[3], out_sem.at[2]).wait()

    f32, bf16 = jnp.float32, jnp.bfloat16
    dma = pltpu.SemaphoreType.DMA
    n_b = len(Y_BATCHES) + 3
    scratch = [
        pltpu.VMEM((rows, embed), bf16), pltpu.VMEM((embed, q_cols), bf16), pltpu.VMEM((2, embed, hd), bf16),
        pltpu.VMEM((q_cols, embed), bf16), pltpu.SMEM((rows,), jnp.int32),
        pltpu.VMEM((RING, GROUP, seq, hd), bf16), pltpu.VMEM((RING, GROUP, seq, hd), bf16),
        pltpu.VMEM((n_groups, GROUP, q_cols), f32), pltpu.VMEM((n_groups, 3, GROUP, q_cols), f32),
        pltpu.VMEM((hd, hd), f32), pltpu.VMEM((GROUP * hd, hd), bf16),
        pltpu.VMEM((2, seq, hd), f32), pltpu.VMEM((hd, hd), f32), pltpu.VMEM((2, 8, hd), f32),
        pltpu.VMEM((rows, hd), f32),
        pltpu.VMEM((rows, hd), bf16), pltpu.VMEM((rows, hd), bf16), pltpu.VMEM((heads_local, rows, hd), f32),
        pltpu.VMEM((hd, seq), bf16),
        pltpu.VMEM((4, last, prow + 8, hd), f32), pltpu.VMEM((last, 3, prow + 8, hd), f32),
        pltpu.VMEM((4, n_pieces, piece_rows + 8, hd), f32), pltpu.VMEM((n_pieces, 3, piece_rows + 8, hd), f32),
        pltpu.VMEM((rows, q_cols), f32), pltpu.VMEM((4, rows, q_cols), f32),
        dma((6,)), dma((RING,)), dma((RING,)), dma((n_pieces,)), dma((3,)), dma((n_groups,)),
        dma((3,)), dma((last,)), dma((3,)), dma((n_pieces,)), dma((3,)), dma((n_b,)), dma((3,)),
    ]
    return kernel, scratch


def store_kernel(y_ref, k_ref, v_ref, yo_ref, ko_ref, vo_ref, y_buf, y16, k_buf, v_buf, sem):
    trips = [(k_ref, k_buf, ko_ref), (v_ref, v_buf, vo_ref)]
    y_in = pltpu.make_async_copy(y_ref, y_buf, sem.at[4])
    y_in.start()
    reads = [pltpu.make_async_copy(a, b, sem.at[i]) for i, (a, b, _) in enumerate(trips)]
    writes = [pltpu.make_async_copy(b, c, sem.at[2 + i]) for i, (_, b, c) in enumerate(trips)]
    for c in reads:
        c.start()
    for r, w in zip(reads, writes):
        r.wait()
        w.start()
    y_in.wait()
    y16[...] = (y_buf[3] + y_buf[0] + y_buf[1] + y_buf[2]).astype(y16.dtype)
    y_w = pltpu.make_async_copy(y16, yo_ref, sem.at[5])
    y_w.start()
    for w in writes + [y_w]:
        w.wait()


def solution(mesh):
    def local_step(hidden, w_query, w_key, w_value, w_out, k_cache, v_cache, lengths):
        rows, embed = hidden.shape
        hd = w_key.shape[1]
        seq = k_cache.shape[1]
        heads_local = w_query.shape[1] // hd
        q_cols = heads_local * hd
        kernel, scratch = make_kernel(rows, embed, seq, heads_local, hd)
        any_spec = pl.BlockSpec(memory_space=pl.ANY)
        outs = (jax.ShapeDtypeStruct((rows, q_cols), jnp.bfloat16),
                jax.ShapeDtypeStruct((rows, hd), jnp.bfloat16),
                jax.ShapeDtypeStruct((rows, hd), jnp.bfloat16))
        raw = pl.pallas_call(
            kernel,
            out_shape=(jax.ShapeDtypeStruct((4, rows, q_cols), jnp.float32),) + outs[1:],
            in_specs=[any_spec] * 8,
            out_specs=(any_spec,) * 3,
            scratch_shapes=scratch,
            compiler_params=pltpu.CompilerParams(
                collective_id=0, has_side_effects=True, vmem_limit_bytes=67043328),
            name="mqa_decode",
        )(hidden, w_query, w_key, w_value, w_out, k_cache, v_cache, lengths)
        return pl.pallas_call(
            store_kernel,
            out_shape=outs,
            in_specs=[any_spec] * 3,
            out_specs=(any_spec,) * 3,
            scratch_shapes=[pltpu.VMEM((4, rows, q_cols), jnp.float32)] + [pltpu.VMEM(o.shape, o.dtype) for o in outs]
            + [pltpu.SemaphoreType.DMA((6,))],
            name="store_outputs",
        )(*raw)

    return jax.shard_map(
        local_step,
        mesh=mesh,
        in_specs=(P('bx', None), P(None, 'sq'), P(None, None), P(None, None), P('sq', None),
                  P('bx', 'sq', None), P('bx', 'sq', None), P('bx')),
        out_specs=(P('bx', 'sq'), P('bx', None), P('bx', None)),
        check_vma=False,
    )
```

```python
import math
import jax
import jax.numpy as jnp
from jax import lax
from jax.experimental import pallas as pl
from jax.experimental.pallas import tpu as pltpu
from jax.sharding import PartitionSpec as P

ROPE_BASE = 10000.0
GROUP = 8
RING = 3
CHUNK = 1024
PIECE = 4
MASKED = -3e38
MESH = pl.DeviceIdType.MESH
Y_BATCHES = {5: (0, 4)}


def make_kernel(rows, embed, seq, heads_local, hd):
    n_groups = rows // GROUP
    n_heads = 4 * heads_local
    assert n_heads * GROUP == hd and hd == 128
    q_cols = heads_local * hd
    last = n_groups - 1
    exp_c = hd ** -0.5 * math.log2(math.e)
    n_pieces = GROUP // PIECE
    piece_rows = heads_local * PIECE
    half = hd // 2
    freqs = [ROPE_BASE ** (-2.0 * i / hd) for i in range(half)]
    prow = heads_local * GROUP

    def kernel(hid_hbm, wq_hbm, wk_hbm, wv_hbm, wo_hbm, k_hbm, v_hbm, len_hbm,
               y_out, kn_out, vn_out,
               hid, wq, wkv, wo, lens_s, kb, vb, qown, qrec, qmat, qblk, sbuf, oacc, mrow,
               vnf, snew, wts, psend, prec, tsend, trec, attn, ysend,
               in_sem, ksem, vsem, tsem, qs_sem, qr_sem, ps_sem, pr_sem, ts_sem, tr_sem, ys_sem, yr_sem):
        bx = lax.axis_index('bx')
        me = lax.axis_index('sq')
        chip, core = me // 2, me % 2
        peers = [chip * 2 + (1 - core), (1 - chip) * 2 + core, (1 - chip) * 2 + (1 - core)]
        far_first = (1, 2, 0)
        base = me * seq

        def cp(src, dst, sem):
            return pltpu.make_async_copy(src, dst, sem)

        def k_copy(g):
            return cp(k_hbm.at[pl.ds(g * GROUP, GROUP)], kb.at[g % RING], ksem.at[g % RING])

        def v_copy(g):
            return cp(v_hbm.at[pl.ds(g * GROUP, GROUP)], vb.at[g % RING], vsem.at[g % RING])

        def v_tail(c):
            r0 = last * GROUP + c * PIECE
            return cp(v_hbm.at[r0:r0 + PIECE], vb.at[last % RING, c * PIECE:(c + 1) * PIECE], tsem.at[c])

        ins = [cp(len_hbm, lens_s, in_sem.at[0]), cp(hid_hbm, hid, in_sem.at[1]), cp(wq_hbm, wq, in_sem.at[2]),
               cp(wk_hbm, wkv.at[0], in_sem.at[3]), cp(wv_hbm, wkv.at[1], in_sem.at[4]), cp(wo_hbm, wo, in_sem.at[5])]
        for c in ins[:5]:
            c.start()
        k_copy(0).start()
        k_copy(1).start()
        v_copy(0).start()

        barrier = pltpu.get_barrier_semaphore()
        for p in peers:
            pl.semaphore_signal(barrier, inc=1, device_id=(bx, p), device_id_type=MESH)

        k_copy(2).start()
        v_copy(1).start()
        ins[5].start()

        lane = lax.broadcasted_iota(jnp.int32, (1, hd), 1)
        lane_i = lane % half
        freq = jnp.zeros((1, hd), jnp.float32)
        for i in range(half):
            freq = jnp.where(lane_i == i, jnp.float32(freqs[i]), freq)
        ins[0].wait()
        sub = lax.broadcasted_iota(jnp.int32, (GROUP, 1), 0)
        pos_rows = []
        for g in range(n_groups):
            t = jnp.zeros((GROUP, 1), jnp.int32)
            for r in range(GROUP):
                t = jnp.where(sub == r, lens_s[g * GROUP + r], t)
            pos_rows.append(t)
        t_col = jnp.concatenate(pos_rows, axis=0).astype(jnp.float32)
        ang = t_col * freq
        cos_t = jnp.cos(ang)
        sin_t = jnp.where(lane < half, -1.0, 1.0) * jnp.sin(ang)

        def rope(x):
            return x * cos_t + pltpu.roll(x, half, 1) * sin_t

        ins[1].wait()
        ins[2].wait()
        qp = jnp.dot(hid[...], wq[...], preferred_element_type=jnp.float32)
        for h in range(heads_local):
            cs = slice(h * hd, (h + 1) * hd)
            q_h = rope(qp[:, cs]).astype(jnp.bfloat16).astype(jnp.float32)
            qown[:, :, cs] = q_h.reshape(n_groups, GROUP, hd)
        pl.semaphore_wait(barrier, 3)

        def q_copy(g, d):
            return pltpu.make_async_remote_copy(
                src_ref=qown.at[g], dst_ref=qrec.at[g, d], send_sem=qs_sem.at[d],
                recv_sem=qr_sem.at[g], device_id=(bx, peers[d]), device_id_type=MESH)

        for g in range(n_groups):
            for d in far_first:
                q_copy(g, d).start()

        ins[3].wait()
        ins[4].wait()
        kn = rope(jnp.dot(hid[...], wkv[0], preferred_element_type=jnp.float32)).astype(jnp.bfloat16)
        vn = jnp.dot(hid[...], wkv[1], preferred_element_type=jnp.float32).astype(jnp.bfloat16)
        kn_out[...] = kn
        vn_out[...] = vn
        knf = kn.astype(jnp.float32)
        vnf[...] = vn.astype(jnp.float32)
        for h in range(heads_local):
            q_h = qown[:, :, h * hd:(h + 1) * hd].reshape(rows, hd)
            s_h = jnp.sum(q_h * knf, axis=1, keepdims=True)
            snew[h] = jnp.broadcast_to(s_h, (rows, hd))

        lane_r = lane // n_heads

        def lens_row(g):
            out = jnp.zeros((1, hd), jnp.int32)
            for r in range(GROUP):
                out = jnp.where(lane_r == r, lens_s[g * GROUP + r], out)
            return out

        def q_wait(g):
            pltpu.make_async_copy(qrec.at[g], qrec.at[g], qr_sem.at[g]).wait()

        def build_q(g):
            for s in range(4):
                for h in range(heads_local):
                    cs = slice(h * hd, (h + 1) * hd)
                    blk = qown[g, :, cs] if s == 3 else qrec[g, s, :, cs]
                    qmat[pl.ds(s * heads_local + h, GROUP, stride=n_heads), :] = blk
            qt = qmat[...].T.astype(jnp.bfloat16)
            for r in range(GROUP):
                qblk[r * hd:(r + 1) * hd, :] = jnp.where(lane_r == r, qt, jnp.zeros_like(qt))

        def scores(g, c, ln):
            sl = slice(c * CHUNK, (c + 1) * CHUNK)
            kc = jnp.concatenate([kb[g % RING, r, sl, :] for r in range(GROUP)], axis=1)
            s = jnp.dot(kc, qblk[...], preferred_element_type=jnp.float32)
            pos = lax.broadcasted_iota(jnp.int32, (CHUNK, hd), 0) + (base + c * CHUNK)
            s = jnp.where(pos < ln, s, MASKED)
            sbuf[g % 2, sl, :] = s
            return jnp.max(s.reshape(CHUNK // 8, 8, hd), axis=0)

        def weights(g, lo, size, mu):
            w = jnp.exp2((sbuf[g % 2, lo:lo + size, :] - mu) * exp_c)
            part = jnp.sum(w.reshape(size // 8, 8, hd), axis=0)
            return w.astype(jnp.bfloat16).T, part

        def weighted(g, r, wt, lo, size):
            vc = jnp.concatenate([vb[g % RING, r + i, lo:lo + size, :] for i in range(2)], axis=1)
            o = jnp.dot(wt, vc, preferred_element_type=jnp.float32)
            return jnp.concatenate([o[:n_heads, :hd], o[n_heads:, hd:]], axis=0)

        def values(g, lo, size, mu):
            wt, part = weights(g, lo, size, mu)
            for r in range(0, GROUP, 2):
                rs = slice(r * n_heads, (r + 2) * n_heads)
                o = weighted(g, r, wt[rs, :], lo, size)
                if lo == 0:
                    oacc[rs, :] = o
                else:
                    oacc[rs, :] += o
            return part

        def keep_max(g, m):
            mrow[g % 2] = jnp.broadcast_to(jnp.max(m, axis=0, keepdims=True), (8, hd))

        def p_copy(g, d):
            return pltpu.make_async_remote_copy(
                src_ref=psend.at[d, g], dst_ref=prec.at[g, d], send_sem=ps_sem.at[d],
                recv_sem=pr_sem.at[g], device_id=(bx, peers[d]), device_id_type=MESH)

        def send_part(g, l):
            for h in range(n_heads):
                k, hh = h // heads_local, h % heads_local
                psend[k, g, hh * GROUP:(hh + 1) * GROUP, :] = oacc[pl.ds(h, GROUP, stride=n_heads), :]
            l_row = jnp.sum(l, axis=0, keepdims=True)
            ml = jnp.where(sub == 0, mrow[g % 2], jnp.where(sub == 1, l_row, 0.0))
            for k in range(4):
                psend[k, g, prow:prow + 8, :] = ml
            for d in far_first:
                p_copy(g, d).start()

        def t_copy(c, d):
            return pltpu.make_async_remote_copy(
                src_ref=tsend.at[d, c], dst_ref=trec.at[c, d], send_sem=ts_sem.at[d],
                recv_sem=tr_sem.at[c], device_id=(bx, peers[d]), device_id_type=MESH)

        def send_piece(c, l_row):
            ml = jnp.where(sub == 0, mrow[last % 2], jnp.where(sub == 1, l_row, 0.0))
            for h in range(n_heads):
                k, hh = h // heads_local, h % heads_local
                tsend[k, c, hh * PIECE:(hh + 1) * PIECE, :] = (
                    oacc[pl.ds(c * PIECE * n_heads + h, PIECE, stride=n_heads), :])
            for k in range(4):
                tsend[k, c, piece_rows:piece_rows + 8, :] = ml
            for d in far_first:
                t_copy(c, d).start()

        def picks(nr, r0):
            row = lax.broadcasted_iota(jnp.int32, (heads_local * nr, hd), 0)
            at = (r0 + row % nr) * n_heads + row // nr
            lane_p = lax.broadcasted_iota(jnp.int32, (heads_local * nr, hd), 1)
            return [lane_p == at + d * heads_local for d in range(4)]

        def combine_rows(parts, row0, nr, picked):
            n = heads_local * nr
            rs = slice(row0, row0 + nr)

            def to_col(d, row):
                return jnp.sum(jnp.where(picked[d], row, 0.0), axis=1, keepdims=True)

            s_new = jnp.concatenate([snew[h, rs, :] for h in range(heads_local)], axis=0)
            ms = [to_col(d, p[n:n + 1, :]) for d, p in enumerate(parts)]
            ls = [to_col(d, p[n + 1:n + 2, :]) for d, p in enumerate(parts)]
            top = s_new
            for m in ms:
                top = jnp.maximum(top, m)
            f_new = jnp.exp2((s_new - top) * exp_c)
            den = f_new
            num = f_new * jnp.concatenate([vnf[rs, :]] * heads_local, axis=0)
            for p, m, l in zip(parts, ms, ls):
                f = jnp.exp2((m - top) * exp_c)
                den = den + f * l
                num = num + f * p[:n, :]
            o = num / den
            for h in range(heads_local):
                attn[rs, h * hd:(h + 1) * hd] = o[h * nr:(h + 1) * nr, :]

        def combine(g):
            parts = [prec[g, d] for d in range(3)] + [psend[3, g]]
            combine_rows(parts, g * GROUP, GROUP, picks(GROUP, 0))

        def combine_piece(c):
            pltpu.make_async_copy(trec.at[c], trec.at[c], tr_sem.at[c]).wait()
            parts = [trec[c, d] for d in range(3)] + [tsend[3, c]]
            combine_rows(parts, last * GROUP + c * PIECE, PIECE, picks(PIECE, c * PIECE))

        def p_wait(g):
            pltpu.make_async_copy(prec.at[g], prec.at[g], pr_sem.at[g]).wait()

        y_batches = []

        def y_copy(b, g0, ng, d):
            sl = pl.ds(g0 * GROUP, ng * GROUP)
            return pltpu.make_async_remote_copy(
                src_ref=ysend.at[d, sl], dst_ref=y_out.at[d, sl], send_sem=ys_sem.at[d],
                recv_sem=yr_sem.at[b], device_id=(bx, peers[d]), device_id_type=MESH)

        def project(g0, ng):
            b = len(y_batches)
            y_batches.append((b, g0, ng))
            sl = slice(g0 * GROUP, (g0 + ng) * GROUP)
            lhs = attn[sl, :].astype(jnp.bfloat16)
            for d in far_first + (3,):
                col = pl.multiple_of((me if d == 3 else peers[d]) * q_cols, q_cols)
                yp = jnp.dot(lhs, wo[:, pl.ds(col, q_cols)], preferred_element_type=jnp.float32)
                if d < 3:
                    ysend[d, sl, :] = yp
                    y_copy(b, g0, ng, d).start()
                else:
                    y_out[3, sl, :] = yp

        def finish(b, g0, ng):
            sl = pl.ds(g0 * GROUP, ng * GROUP)
            pltpu.make_async_copy(y_out.at[0:3, sl], y_out.at[0:3, sl], yr_sem.at[b]).wait()

        q_wait(0)
        build_q(0)
        k_copy(0).wait()
        ln = lens_row(0)
        m = jnp.full((8, hd), MASKED, jnp.float32)
        for c in range(seq // CHUNK):
            m = jnp.maximum(m, scores(0, c, ln))
        keep_max(0, m)

        def shift(g):
            return jnp.where(lens_row(g) > base, mrow[g % 2, 0:1, :], 0.0)

        for g in range(last - 1):
            if g + 3 < n_groups:
                k_copy(g + 3).start()
            if g + 2 < last:
                v_copy(g + 2).start()
            if g + 2 == last:
                for c in range(n_pieces):
                    v_tail(c).start()
            q_wait(g + 1)
            if g >= 2:
                p_wait(g - 2)
            if g == 3:
                ins[5].wait()
            k_copy(g + 1).wait()
            v_copy(g).wait()
            build_q(g + 1)
            mu = shift(g)
            ln = lens_row(g + 1)
            m = jnp.full((8, hd), MASKED, jnp.float32)
            l = jnp.zeros((8, hd), jnp.float32)
            for c in range(seq // CHUNK):
                l = l + values(g, c * CHUNK, CHUNK, mu)
                m = jnp.maximum(m, scores(g + 1, c, ln))
            keep_max(g + 1, m)
            send_part(g, l)
            if g >= 2:
                combine(g - 2)
            if g in Y_BATCHES:
                project(*Y_BATCHES[g])

        pre = last - 1
        q_wait(last)
        p_wait(pre - 2)
        k_copy(last).wait()
        build_q(last)
        ln = lens_row(last)
        m = jnp.full((8, hd), MASKED, jnp.float32)
        for c in range(seq // CHUNK):
            m = jnp.maximum(m, scores(last, c, ln))
        keep_max(last, m)
        combine(pre - 2)
        mu = shift(pre)
        v_copy(pre).wait()
        l = jnp.zeros((8, hd), jnp.float32)
        for c in range(seq // CHUNK):
            l = l + values(pre, c * CHUNK, CHUNK, mu)
        send_part(pre, l)
        mu = shift(last)
        l = jnp.zeros((8, hd), jnp.float32)
        for c in range(seq // CHUNK):
            wt, part = weights(last, c * CHUNK, CHUNK, mu)
            wts[:, c * CHUNK:(c + 1) * CHUNK] = wt
            l = l + part
        l_row = jnp.sum(l, axis=0, keepdims=True)
        for c in range(n_pieces):
            v_tail(c).wait()
            for r in range(c * PIECE, (c + 1) * PIECE, 2):
                rs = slice(r * n_heads, (r + 2) * n_heads)
                oacc[rs, :] = weighted(last, r, wts[rs, :], 0, seq)
            send_piece(c, l_row)
        p_wait(pre - 1)
        combine(pre - 1)
        project(pre - 2, 2)
        p_wait(pre)
        combine(pre)
        project(pre, 1)
        for c in range(n_pieces):
            combine_piece(c)
        project(last, 1)
        for b in y_batches:
            finish(*b)
        for d in range(3):
            pltpu.make_async_copy(qown, qown, qs_sem.at[d]).wait()
            pltpu.make_async_copy(psend.at[d], psend.at[d], ps_sem.at[d]).wait()
            pltpu.make_async_copy(tsend.at[d], tsend.at[d], ts_sem.at[d]).wait()
            pltpu.make_async_copy(ysend.at[d], ysend.at[d], ys_sem.at[d]).wait()

    f32, bf16 = jnp.float32, jnp.bfloat16
    dma = pltpu.SemaphoreType.DMA
    n_b = len(Y_BATCHES) + 3
    scratch = [
        pltpu.VMEM((rows, embed), bf16), pltpu.VMEM((embed, q_cols), bf16), pltpu.VMEM((2, embed, hd), bf16),
        pltpu.VMEM((q_cols, embed), bf16), pltpu.SMEM((rows,), jnp.int32),
        pltpu.VMEM((RING, GROUP, seq, hd), bf16), pltpu.VMEM((RING, GROUP, seq, hd), bf16),
        pltpu.VMEM((n_groups, GROUP, q_cols), f32), pltpu.VMEM((n_groups, 3, GROUP, q_cols), f32),
        pltpu.VMEM((hd, hd), f32), pltpu.VMEM((GROUP * hd, hd), bf16),
        pltpu.VMEM((2, seq, hd), f32), pltpu.VMEM((hd, hd), f32), pltpu.VMEM((2, 8, hd), f32),
        pltpu.VMEM((rows, hd), f32),
        pltpu.VMEM((heads_local, rows, hd), f32),
        pltpu.VMEM((hd, seq), bf16),
        pltpu.VMEM((4, last, prow + 8, hd), f32), pltpu.VMEM((last, 3, prow + 8, hd), f32),
        pltpu.VMEM((4, n_pieces, piece_rows + 8, hd), f32), pltpu.VMEM((n_pieces, 3, piece_rows + 8, hd), f32),
        pltpu.VMEM((rows, q_cols), f32), pltpu.VMEM((3, rows, q_cols), f32),
        dma((6,)), dma((RING,)), dma((RING,)), dma((n_pieces,)), dma((3,)), dma((n_groups,)),
        dma((3,)), dma((last,)), dma((3,)), dma((n_pieces,)), dma((3,)), dma((n_b,)),
    ]
    return kernel, scratch


def store_kernel(y_ref, k_ref, v_ref, yo_ref, ko_ref, vo_ref, y16, sem):
    y16[...] = (y_ref[3] + y_ref[0] + y_ref[1] + y_ref[2]).astype(y16.dtype)
    writes = [pltpu.make_async_copy(a, b, sem.at[i])
              for i, (a, b) in enumerate(((y16, yo_ref), (k_ref, ko_ref), (v_ref, vo_ref)))]
    for w in writes:
        w.start()
    for w in writes:
        w.wait()


def solution(mesh):
    def local_step(hidden, w_query, w_key, w_value, w_out, k_cache, v_cache, lengths):
        rows, embed = hidden.shape
        hd = w_key.shape[1]
        seq = k_cache.shape[1]
        heads_local = w_query.shape[1] // hd
        q_cols = heads_local * hd
        kernel, scratch = make_kernel(rows, embed, seq, heads_local, hd)
        any_spec = pl.BlockSpec(memory_space=pl.ANY)
        vmem_spec = pl.BlockSpec(memory_space=pltpu.VMEM)
        outs = (jax.ShapeDtypeStruct((rows, q_cols), jnp.bfloat16),
                jax.ShapeDtypeStruct((rows, hd), jnp.bfloat16),
                jax.ShapeDtypeStruct((rows, hd), jnp.bfloat16))
        raw = pl.pallas_call(
            kernel,
            out_shape=tuple(pltpu.VMEM(sh, dt) for sh, dt in (((4, rows, q_cols), jnp.float32),
                                                              ((rows, hd), jnp.bfloat16), ((rows, hd), jnp.bfloat16))),
            in_specs=[any_spec] * 8,
            out_specs=(vmem_spec,) * 3,
            scratch_shapes=scratch,
            compiler_params=pltpu.CompilerParams(
                collective_id=0, has_side_effects=True, vmem_limit_bytes=66300000),
            name="mqa_decode",
        )(hidden, w_query, w_key, w_value, w_out, k_cache, v_cache, lengths)
        return pl.pallas_call(
            store_kernel,
            out_shape=outs,
            in_specs=[vmem_spec] * 3,
            out_specs=(any_spec,) * 3,
            scratch_shapes=[pltpu.VMEM(outs[0].shape, outs[0].dtype), pltpu.SemaphoreType.DMA((3,))],
            name="store_outputs",
        )(*[pltpu.with_memory_space_constraint(r, pltpu.VMEM) for r in raw])

    return jax.shard_map(
        local_step,
        mesh=mesh,
        in_specs=(P('bx', None), P(None, 'sq'), P(None, None), P(None, None), P('sq', None),
                  P('bx', 'sq', None), P('bx', 'sq', None), P('bx')),
        out_specs=(P('bx', 'sq'), P('bx', None), P('bx', None)),
        check_vma=False,
    )
```

```python
import math
import jax
import jax.numpy as jnp
from jax import lax
from jax.experimental import pallas as pl
from jax.experimental.pallas import tpu as pltpu
from jax.sharding import PartitionSpec as P

ROPE_BASE = 10000.0
GROUP = 8
RING = 3
CHUNK = 1024
PIECE = 4
MASKED = -3e38
MESH = pl.DeviceIdType.MESH
Y_BATCHES = {3: (0, 2), 5: (2, 2)}


def make_kernel(rows, embed, seq, heads_local, hd):
    n_groups = rows // GROUP
    n_heads = 4 * heads_local
    assert n_heads * GROUP == hd and hd == 128
    q_cols = heads_local * hd
    last = n_groups - 1
    exp_c = hd ** -0.5 * math.log2(math.e)
    n_pieces = GROUP // PIECE
    piece_rows = heads_local * PIECE
    half = hd // 2
    freqs = [ROPE_BASE ** (-2.0 * i / hd) for i in range(half)]
    prow = heads_local * GROUP

    def kernel(hid_hbm, wq_hbm, wk_hbm, wv_hbm, wo_hbm, k_hbm, v_hbm, len_hbm,
               y_out, kn_out, vn_out,
               hid, wq, wkv, wo, lens_s, kb, vb, qown, qrec, qmat, qblk, sbuf, oacc, mrow,
               vnf, snew, wts, psend, prec, tsend, trec, attn, ysend,
               in_sem, ksem, vsem, tsem, qs_sem, qr_sem, ps_sem, pr_sem, ts_sem, tr_sem, ys_sem, yr_sem):
        bx = lax.axis_index('bx')
        me = lax.axis_index('sq')
        chip, core = me // 2, me % 2
        peers = [chip * 2 + (1 - core), (1 - chip) * 2 + core, (1 - chip) * 2 + (1 - core)]
        far_first = (1, 2, 0)
        base = me * seq

        def cp(src, dst, sem):
            return pltpu.make_async_copy(src, dst, sem)

        def k_copy(g):
            return cp(k_hbm.at[pl.ds(g * GROUP, GROUP)], kb.at[g % RING], ksem.at[g % RING])

        def v_copy(g):
            return cp(v_hbm.at[pl.ds(g * GROUP, GROUP)], vb.at[g % RING], vsem.at[g % RING])

        def v_tail(c):
            r0 = last * GROUP + c * PIECE
            return cp(v_hbm.at[r0:r0 + PIECE], vb.at[last % RING, c * PIECE:(c + 1) * PIECE], tsem.at[c])

        ins = [cp(len_hbm, lens_s, in_sem.at[0]), cp(hid_hbm, hid, in_sem.at[1]), cp(wq_hbm, wq, in_sem.at[2]),
               cp(wk_hbm, wkv.at[0], in_sem.at[3]), cp(wv_hbm, wkv.at[1], in_sem.at[4]), cp(wo_hbm, wo, in_sem.at[5])]
        for c in ins[:5]:
            c.start()
        k_copy(0).start()
        k_copy(1).start()
        v_copy(0).start()

        barrier = pltpu.get_barrier_semaphore()
        for p in peers:
            pl.semaphore_signal(barrier, inc=1, device_id=(bx, p), device_id_type=MESH)

        k_copy(2).start()
        v_copy(1).start()
        ins[5].start()

        lane = lax.broadcasted_iota(jnp.int32, (1, hd), 1)
        lane_i = lane % half
        freq = jnp.zeros((1, hd), jnp.float32)
        for i in range(half):
            freq = jnp.where(lane_i == i, jnp.float32(freqs[i]), freq)
        ins[0].wait()
        sub = lax.broadcasted_iota(jnp.int32, (GROUP, 1), 0)
        pos_rows = []
        for g in range(n_groups):
            t = jnp.zeros((GROUP, 1), jnp.int32)
            for r in range(GROUP):
                t = jnp.where(sub == r, lens_s[g * GROUP + r], t)
            pos_rows.append(t)
        t_col = jnp.concatenate(pos_rows, axis=0).astype(jnp.float32)
        ang = t_col * freq
        cos_t = jnp.cos(ang)
        sin_t = jnp.where(lane < half, -1.0, 1.0) * jnp.sin(ang)

        def rope(x):
            return x * cos_t + pltpu.roll(x, half, 1) * sin_t

        ins[1].wait()
        ins[2].wait()
        qp = jnp.dot(hid[...], wq[...], preferred_element_type=jnp.float32)
        for h in range(heads_local):
            cs = slice(h * hd, (h + 1) * hd)
            q_h = rope(qp[:, cs]).astype(jnp.bfloat16).astype(jnp.float32)
            qown[:, :, cs] = q_h.reshape(n_groups, GROUP, hd)
        pl.semaphore_wait(barrier, 3)

        def q_copy(g, d):
            return pltpu.make_async_remote_copy(
                src_ref=qown.at[g], dst_ref=qrec.at[g, d], send_sem=qs_sem.at[d],
                recv_sem=qr_sem.at[g], device_id=(bx, peers[d]), device_id_type=MESH)

        for g in range(n_groups):
            for d in far_first:
                q_copy(g, d).start()

        ins[3].wait()
        ins[4].wait()
        kn = rope(jnp.dot(hid[...], wkv[0], preferred_element_type=jnp.float32)).astype(jnp.bfloat16)
        vn = jnp.dot(hid[...], wkv[1], preferred_element_type=jnp.float32).astype(jnp.bfloat16)
        kn_out[...] = kn
        vn_out[...] = vn
        knf = kn.astype(jnp.float32)
        vnf[...] = vn.astype(jnp.float32)
        for h in range(heads_local):
            q_h = qown[:, :, h * hd:(h + 1) * hd].reshape(rows, hd)
            s_h = jnp.sum(q_h * knf, axis=1, keepdims=True)
            snew[h] = jnp.broadcast_to(s_h, (rows, hd))

        lane_r = lane // n_heads

        def lens_row(g):
            out = jnp.zeros((1, hd), jnp.int32)
            for r in range(GROUP):
                out = jnp.where(lane_r == r, lens_s[g * GROUP + r], out)
            return out

        def q_wait(g):
            pltpu.make_async_copy(qrec.at[g], qrec.at[g], qr_sem.at[g]).wait()

        def build_q(g):
            for s in range(4):
                for h in range(heads_local):
                    cs = slice(h * hd, (h + 1) * hd)
                    blk = qown[g, :, cs] if s == 3 else qrec[g, s, :, cs]
                    qmat[pl.ds(s * heads_local + h, GROUP, stride=n_heads), :] = blk
            qt = qmat[...].T.astype(jnp.bfloat16)
            for r in range(GROUP):
                qblk[r * hd:(r + 1) * hd, :] = jnp.where(lane_r == r, qt, jnp.zeros_like(qt))

        def scores(g, c, ln):
            sl = slice(c * CHUNK, (c + 1) * CHUNK)
            kc = jnp.concatenate([kb[g % RING, r, sl, :] for r in range(GROUP)], axis=1)
            s = jnp.dot(kc, qblk[...], preferred_element_type=jnp.float32)
            pos = lax.broadcasted_iota(jnp.int32, (CHUNK, hd), 0) + (base + c * CHUNK)
            s = jnp.where(pos < ln, s, MASKED)
            sbuf[g % 2, sl, :] = s
            return jnp.max(s.reshape(CHUNK // 8, 8, hd), axis=0)

        def weights(g, lo, size, mu):
            w = jnp.exp2((sbuf[g % 2, lo:lo + size, :] - mu) * exp_c)
            part = jnp.sum(w.reshape(size // 8, 8, hd), axis=0)
            return w.astype(jnp.bfloat16).T, part

        def weighted(g, r, wt, lo, size):
            vc = jnp.concatenate([vb[g % RING, r + i, lo:lo + size, :] for i in range(2)], axis=1)
            o = jnp.dot(wt, vc, preferred_element_type=jnp.float32)
            return jnp.concatenate([o[:n_heads, :hd], o[n_heads:, hd:]], axis=0)

        def values(g, lo, size, mu):
            wt, part = weights(g, lo, size, mu)
            for r in range(0, GROUP, 2):
                rs = slice(r * n_heads, (r + 2) * n_heads)
                o = weighted(g, r, wt[rs, :], lo, size)
                if lo == 0:
                    oacc[rs, :] = o
                else:
                    oacc[rs, :] += o
            return part

        def keep_max(g, m):
            mrow[g % 2] = jnp.broadcast_to(jnp.max(m, axis=0, keepdims=True), (8, hd))

        def p_copy(g, d):
            return pltpu.make_async_remote_copy(
                src_ref=psend.at[d, g], dst_ref=prec.at[g, d], send_sem=ps_sem.at[d],
                recv_sem=pr_sem.at[g], device_id=(bx, peers[d]), device_id_type=MESH)

        def send_part(g, l):
            for h in range(n_heads):
                k, hh = h // heads_local, h % heads_local
                psend[k, g, hh * GROUP:(hh + 1) * GROUP, :] = oacc[pl.ds(h, GROUP, stride=n_heads), :]
            l_row = jnp.sum(l, axis=0, keepdims=True)
            ml = jnp.where(sub == 0, mrow[g % 2], jnp.where(sub == 1, l_row, 0.0))
            for k in range(4):
                psend[k, g, prow:prow + 8, :] = ml
            for d in far_first:
                p_copy(g, d).start()

        def t_copy(c, d):
            return pltpu.make_async_remote_copy(
                src_ref=tsend.at[d, c], dst_ref=trec.at[c, d], send_sem=ts_sem.at[d],
                recv_sem=tr_sem.at[c], device_id=(bx, peers[d]), device_id_type=MESH)

        def send_piece(c, l_row):
            ml = jnp.where(sub == 0, mrow[last % 2], jnp.where(sub == 1, l_row, 0.0))
            for h in range(n_heads):
                k, hh = h // heads_local, h % heads_local
                tsend[k, c, hh * PIECE:(hh + 1) * PIECE, :] = (
                    oacc[pl.ds(c * PIECE * n_heads + h, PIECE, stride=n_heads), :])
            for k in range(4):
                tsend[k, c, piece_rows:piece_rows + 8, :] = ml
            for d in far_first:
                t_copy(c, d).start()

        def picks(nr, r0):
            row = lax.broadcasted_iota(jnp.int32, (heads_local * nr, hd), 0)
            at = (r0 + row % nr) * n_heads + row // nr
            lane_p = lax.broadcasted_iota(jnp.int32, (heads_local * nr, hd), 1)
            return [lane_p == at + d * heads_local for d in range(4)]

        def combine_rows(parts, row0, nr, picked):
            n = heads_local * nr
            rs = slice(row0, row0 + nr)

            def to_col(d, row):
                return jnp.sum(jnp.where(picked[d], row, 0.0), axis=1, keepdims=True)

            s_new = jnp.concatenate([snew[h, rs, :] for h in range(heads_local)], axis=0)
            ms = [to_col(d, p[n:n + 1, :]) for d, p in enumerate(parts)]
            ls = [to_col(d, p[n + 1:n + 2, :]) for d, p in enumerate(parts)]
            top = s_new
            for m in ms:
                top = jnp.maximum(top, m)
            f_new = jnp.exp2((s_new - top) * exp_c)
            den = f_new
            num = f_new * jnp.concatenate([vnf[rs, :]] * heads_local, axis=0)
            for p, m, l in zip(parts, ms, ls):
                f = jnp.exp2((m - top) * exp_c)
                den = den + f * l
                num = num + f * p[:n, :]
            o = num / den
            for h in range(heads_local):
                attn[rs, h * hd:(h + 1) * hd] = o[h * nr:(h + 1) * nr, :]

        def combine(g):
            parts = [prec[g, d] for d in range(3)] + [psend[3, g]]
            combine_rows(parts, g * GROUP, GROUP, picks(GROUP, 0))

        def combine_piece(c):
            pltpu.make_async_copy(trec.at[c], trec.at[c], tr_sem.at[c]).wait()
            parts = [trec[c, d] for d in range(3)] + [tsend[3, c]]
            combine_rows(parts, last * GROUP + c * PIECE, PIECE, picks(PIECE, c * PIECE))

        def p_wait(g):
            pltpu.make_async_copy(prec.at[g], prec.at[g], pr_sem.at[g]).wait()

        y_batches = []

        def y_copy(b, g0, ng, d):
            sl = pl.ds(g0 * GROUP, ng * GROUP)
            return pltpu.make_async_remote_copy(
                src_ref=ysend.at[peers[d], sl], dst_ref=y_out.at[d, sl], send_sem=ys_sem.at[d],
                recv_sem=yr_sem.at[b], device_id=(bx, peers[d]), device_id_type=MESH)

        def project(g0, ng):
            b = len(y_batches)
            y_batches.append((b, g0, ng))
            sl = slice(g0 * GROUP, (g0 + ng) * GROUP)
            yp = jnp.dot(attn[sl, :].astype(jnp.bfloat16), wo[...], preferred_element_type=jnp.float32)
            for k in range(4):
                ysend[k, sl, :] = yp[:, k * q_cols:(k + 1) * q_cols]
            for d in far_first:
                y_copy(b, g0, ng, d).start()
            y_out[3, sl, :] = ysend[me, sl, :]

        def finish(b, g0, ng):
            sl = pl.ds(g0 * GROUP, ng * GROUP)
            pltpu.make_async_copy(y_out.at[0:3, sl], y_out.at[0:3, sl], yr_sem.at[b]).wait()

        q_wait(0)
        build_q(0)
        k_copy(0).wait()
        ln = lens_row(0)
        m = jnp.full((8, hd), MASKED, jnp.float32)
        for c in range(seq // CHUNK):
            m = jnp.maximum(m, scores(0, c, ln))
        keep_max(0, m)

        def shift(g):
            return jnp.where(lens_row(g) > base, mrow[g % 2, 0:1, :], 0.0)

        for g in range(last - 1):
            if g + 3 < n_groups:
                k_copy(g + 3).start()
            if g + 2 < last:
                v_copy(g + 2).start()
            if g + 2 == last:
                for c in range(n_pieces):
                    v_tail(c).start()
            q_wait(g + 1)
            if g >= 2:
                p_wait(g - 2)
            if g == 3:
                ins[5].wait()
            k_copy(g + 1).wait()
            v_copy(g).wait()
            build_q(g + 1)
            mu = shift(g)
            ln = lens_row(g + 1)
            m = jnp.full((8, hd), MASKED, jnp.float32)
            l = jnp.zeros((8, hd), jnp.float32)
            for c in range(seq // CHUNK):
                l = l + values(g, c * CHUNK, CHUNK, mu)
                m = jnp.maximum(m, scores(g + 1, c, ln))
            keep_max(g + 1, m)
            send_part(g, l)
            if g >= 2:
                combine(g - 2)
            if g in Y_BATCHES:
                project(*Y_BATCHES[g])

        pre = last - 1
        q_wait(last)
        p_wait(pre - 2)
        k_copy(last).wait()
        build_q(last)
        ln = lens_row(last)
        m = jnp.full((8, hd), MASKED, jnp.float32)
        for c in range(seq // CHUNK):
            m = jnp.maximum(m, scores(last, c, ln))
        keep_max(last, m)
        combine(pre - 2)
        mu = shift(pre)
        v_copy(pre).wait()
        l = jnp.zeros((8, hd), jnp.float32)
        for c in range(seq // CHUNK):
            l = l + values(pre, c * CHUNK, CHUNK, mu)
        send_part(pre, l)
        mu = shift(last)
        l = jnp.zeros((8, hd), jnp.float32)
        for c in range(seq // CHUNK):
            wt, part = weights(last, c * CHUNK, CHUNK, mu)
            wts[:, c * CHUNK:(c + 1) * CHUNK] = wt
            l = l + part
        l_row = jnp.sum(l, axis=0, keepdims=True)
        for c in range(n_pieces):
            v_tail(c).wait()
            for r in range(c * PIECE, (c + 1) * PIECE, 2):
                rs = slice(r * n_heads, (r + 2) * n_heads)
                oacc[rs, :] = weighted(last, r, wts[rs, :], 0, seq)
            send_piece(c, l_row)
        p_wait(pre - 1)
        combine(pre - 1)
        project(pre - 2, 2)
        p_wait(pre)
        combine(pre)
        project(pre, 1)
        for c in range(n_pieces):
            combine_piece(c)
        project(last, 1)
        for b in y_batches:
            finish(*b)
        for d in range(3):
            pltpu.make_async_copy(qown, qown, qs_sem.at[d]).wait()
            pltpu.make_async_copy(psend.at[d], psend.at[d], ps_sem.at[d]).wait()
            pltpu.make_async_copy(tsend.at[d], tsend.at[d], ts_sem.at[d]).wait()
            pltpu.make_async_copy(ysend.at[d], ysend.at[d], ys_sem.at[d]).wait()

    f32, bf16 = jnp.float32, jnp.bfloat16
    dma = pltpu.SemaphoreType.DMA
    n_b = len(Y_BATCHES) + 3
    scratch = [
        pltpu.VMEM((rows, embed), bf16), pltpu.VMEM((embed, q_cols), bf16), pltpu.VMEM((2, embed, hd), bf16),
        pltpu.VMEM((q_cols, embed), bf16), pltpu.SMEM((rows,), jnp.int32),
        pltpu.VMEM((RING, GROUP, seq, hd), bf16), pltpu.VMEM((RING, GROUP, seq, hd), bf16),
        pltpu.VMEM((n_groups, GROUP, q_cols), f32), pltpu.VMEM((n_groups, 3, GROUP, q_cols), f32),
        pltpu.VMEM((hd, hd), f32), pltpu.VMEM((GROUP * hd, hd), bf16),
        pltpu.VMEM((2, seq, hd), f32), pltpu.VMEM((hd, hd), f32), pltpu.VMEM((2, 8, hd), f32),
        pltpu.VMEM((rows, hd), f32),
        pltpu.VMEM((heads_local, rows, hd), f32),
        pltpu.VMEM((hd, seq), bf16),
        pltpu.VMEM((4, last, prow + 8, hd), f32), pltpu.VMEM((last, 3, prow + 8, hd), f32),
        pltpu.VMEM((4, n_pieces, piece_rows + 8, hd), f32), pltpu.VMEM((n_pieces, 3, piece_rows + 8, hd), f32),
        pltpu.VMEM((rows, q_cols), f32), pltpu.VMEM((4, rows, q_cols), f32),
        dma((6,)), dma((RING,)), dma((RING,)), dma((n_pieces,)), dma((3,)), dma((n_groups,)),
        dma((3,)), dma((last,)), dma((3,)), dma((n_pieces,)), dma((3,)), dma((n_b,)),
    ]
    return kernel, scratch


def store_kernel(y_ref, k_ref, v_ref, yo_ref, ko_ref, vo_ref, y16, sem):
    y16[...] = (y_ref[3] + y_ref[0] + y_ref[1] + y_ref[2]).astype(y16.dtype)
    writes = [pltpu.make_async_copy(a, b, sem.at[i])
              for i, (a, b) in enumerate(((y16, yo_ref), (k_ref, ko_ref), (v_ref, vo_ref)))]
    for w in writes:
        w.start()
    for w in writes:
        w.wait()


def solution(mesh):
    def local_step(hidden, w_query, w_key, w_value, w_out, k_cache, v_cache, lengths):
        rows, embed = hidden.shape
        hd = w_key.shape[1]
        seq = k_cache.shape[1]
        heads_local = w_query.shape[1] // hd
        q_cols = heads_local * hd
        kernel, scratch = make_kernel(rows, embed, seq, heads_local, hd)
        any_spec = pl.BlockSpec(memory_space=pl.ANY)
        vmem_spec = pl.BlockSpec(memory_space=pltpu.VMEM)
        outs = (jax.ShapeDtypeStruct((rows, q_cols), jnp.bfloat16),
                jax.ShapeDtypeStruct((rows, hd), jnp.bfloat16),
                jax.ShapeDtypeStruct((rows, hd), jnp.bfloat16))
        raw = pl.pallas_call(
            kernel,
            out_shape=tuple(pltpu.VMEM(sh, dt) for sh, dt in (((4, rows, q_cols), jnp.float32),
                                                              ((rows, hd), jnp.bfloat16), ((rows, hd), jnp.bfloat16))),
            in_specs=[any_spec] * 8,
            out_specs=(vmem_spec,) * 3,
            scratch_shapes=scratch,
            compiler_params=pltpu.CompilerParams(
                collective_id=0, has_side_effects=True, vmem_limit_bytes=66300000),
            name="mqa_decode",
        )(hidden, w_query, w_key, w_value, w_out, k_cache, v_cache, lengths)
        return pl.pallas_call(
            store_kernel,
            out_shape=outs,
            in_specs=[vmem_spec] * 3,
            out_specs=(any_spec,) * 3,
            scratch_shapes=[pltpu.VMEM(outs[0].shape, outs[0].dtype), pltpu.SemaphoreType.DMA((3,))],
            name="store_outputs",
        )(*[pltpu.with_memory_space_constraint(r, pltpu.VMEM) for r in raw])

    return jax.shard_map(
        local_step,
        mesh=mesh,
        in_specs=(P('bx', None), P(None, 'sq'), P(None, None), P(None, None), P('sq', None),
                  P('bx', 'sq', None), P('bx', 'sq', None), P('bx')),
        out_specs=(P('bx', 'sq'), P('bx', None), P('bx', None)),
        check_vma=False,
    )
```

```python
import math
import jax
import jax.numpy as jnp
from jax import lax
from jax.experimental import pallas as pl
from jax.experimental.pallas import tpu as pltpu
from jax.sharding import PartitionSpec as P

ROPE_BASE = 10000.0
GROUP = 8
RING = 3
CHUNK = 512
PIECE = 4
MASKED = -3e38
MESH = pl.DeviceIdType.MESH
Y_BATCHES = {3: (0, 2), 4: (2, 1)}


def make_kernel(rows, embed, seq, heads_local, hd):
    n_groups = rows // GROUP
    n_heads = 4 * heads_local
    assert n_heads * GROUP == hd and hd == 128
    q_cols = heads_local * hd
    last = n_groups - 1
    exp_c = hd ** -0.5 * math.log2(math.e)
    n_pieces = GROUP // PIECE
    piece_rows = heads_local * PIECE
    half = hd // 2
    freqs = [ROPE_BASE ** (-2.0 * i / hd) for i in range(half)]
    prow = heads_local * GROUP

    def kernel(hid_hbm, wq_hbm, wk_hbm, wv_hbm, wo_hbm, k_hbm, v_hbm, len_hbm,
               y_out, kn_out, vn_out,
               hid, wq, wkv, wo, lens_s, kb, vb, qown, qrec, qmat, qblk, k_turn, sbuf, oacc, mrow,
               vnf, snew, wts, psend, prec, tsend, trec, attn, ysend,
               in_sem, ksem, vsem, tsem, qs_sem, qr_sem, ps_sem, pr_sem, ts_sem, tr_sem, ys_sem, yr_sem):
        bx = lax.axis_index('bx')
        me = lax.axis_index('sq')
        chip, core = me // 2, me % 2
        peers = [chip * 2 + (1 - core), (1 - chip) * 2 + core, (1 - chip) * 2 + (1 - core)]
        far_first = (1, 2, 0)
        base = me * seq

        def cp(src, dst, sem):
            return pltpu.make_async_copy(src, dst, sem)

        def k_copy(g):
            return cp(k_hbm.at[pl.ds(g * GROUP, GROUP)], kb.at[g % RING], ksem.at[g % RING])

        def v_copy(g):
            return cp(v_hbm.at[pl.ds(g * GROUP, GROUP)], vb.at[g % RING], vsem.at[g % RING])

        def v_tail(c):
            r0 = last * GROUP + c * PIECE
            return cp(v_hbm.at[r0:r0 + PIECE], vb.at[last % RING, c * PIECE:(c + 1) * PIECE], tsem.at[c])

        ins = [cp(len_hbm, lens_s, in_sem.at[0]), cp(hid_hbm, hid, in_sem.at[1]), cp(wq_hbm, wq, in_sem.at[2]),
               cp(wk_hbm, wkv.at[0], in_sem.at[3]), cp(wv_hbm, wkv.at[1], in_sem.at[4]), cp(wo_hbm, wo, in_sem.at[5])]
        for c in ins[:5]:
            c.start()
        k_copy(0).start()
        k_copy(1).start()
        v_copy(0).start()

        barrier = pltpu.get_barrier_semaphore()
        for p in peers:
            pl.semaphore_signal(barrier, inc=1, device_id=(bx, p), device_id_type=MESH)

        k_copy(2).start()
        v_copy(1).start()
        ins[5].start()

        lane = lax.broadcasted_iota(jnp.int32, (1, hd), 1)
        lane_i = lane % half
        freq = jnp.zeros((1, hd), jnp.float32)
        for i in range(half):
            freq = jnp.where(lane_i == i, jnp.float32(freqs[i]), freq)
        ins[0].wait()
        sub = lax.broadcasted_iota(jnp.int32, (GROUP, 1), 0)
        pos_rows = []
        for g in range(n_groups):
            t = jnp.zeros((GROUP, 1), jnp.int32)
            for r in range(GROUP):
                t = jnp.where(sub == r, lens_s[g * GROUP + r], t)
            pos_rows.append(t)
        t_col = jnp.concatenate(pos_rows, axis=0).astype(jnp.float32)
        ang = t_col * freq
        cos_t = jnp.cos(ang)
        sin_t = jnp.where(lane < half, -1.0, 1.0) * jnp.sin(ang)

        def rope(x):
            return x * cos_t + pltpu.roll(x, half, 1) * sin_t

        ins[1].wait()
        ins[2].wait()
        qp = jnp.dot(hid[...], wq[...], preferred_element_type=jnp.float32)
        for h in range(heads_local):
            cs = slice(h * hd, (h + 1) * hd)
            q_h = rope(qp[:, cs]).astype(jnp.bfloat16).astype(jnp.float32)
            qown[:, :, cs] = q_h.reshape(n_groups, GROUP, hd)
        pl.semaphore_wait(barrier, 3)

        def q_copy(g, d):
            return pltpu.make_async_remote_copy(
                src_ref=qown.at[g], dst_ref=qrec.at[g, d], send_sem=qs_sem.at[d],
                recv_sem=qr_sem.at[g], device_id=(bx, peers[d]), device_id_type=MESH)

        for g in range(n_groups):
            for d in far_first:
                q_copy(g, d).start()

        ins[3].wait()
        ins[4].wait()
        kn = rope(jnp.dot(hid[...], wkv[0], preferred_element_type=jnp.float32)).astype(jnp.bfloat16)
        vn = jnp.dot(hid[...], wkv[1], preferred_element_type=jnp.float32).astype(jnp.bfloat16)
        kn_out[...] = kn
        vn_out[...] = vn
        knf = kn.astype(jnp.float32)
        vnf[...] = vn.astype(jnp.float32)
        for h in range(heads_local):
            q_h = qown[:, :, h * hd:(h + 1) * hd].reshape(rows, hd)
            s_h = jnp.sum(q_h * knf, axis=1, keepdims=True)
            snew[h] = jnp.broadcast_to(s_h, (rows, hd))

        def per_row(g, vals):
            return jnp.concatenate([jnp.full((n_heads, 1), vals(g * GROUP + r), jnp.int32) for r in range(GROUP)], axis=0)

        def lens_col(g):
            return per_row(g, lambda b: lens_s[b])

        qblk[...] = jnp.zeros_like(qblk)

        def q_wait(g):
            pltpu.make_async_copy(qrec.at[g], qrec.at[g], qr_sem.at[g]).wait()

        def build_q(g):
            for s in range(4):
                for h in range(heads_local):
                    cs = slice(h * hd, (h + 1) * hd)
                    blk = qown[g, :, cs] if s == 3 else qrec[g, s, :, cs]
                    qmat[pl.ds(s * heads_local + h, GROUP, stride=n_heads), :] = blk
            for r in range(GROUP):
                rs = slice(r * n_heads, (r + 1) * n_heads)
                qblk[rs, (r % 2) * hd:(r % 2 + 1) * hd] = qmat[rs, :].astype(jnp.bfloat16)

        def fold(x, op):
            out = x[:, :hd]
            for i in range(1, x.shape[1] // hd):
                out = op(out, x[:, i * hd:(i + 1) * hd])
            return out

        def score_tile(g, t, lo, ln, m, turn=True):
            rs = slice(2 * t * n_heads, (2 * t + 2) * n_heads)
            kc = jnp.concatenate([kb[g % RING, 2 * t + i, lo:lo + CHUNK, :] for i in range(2)], axis=1)
            if turn:
                k_turn[t % 2] = kc.T
                kt = k_turn[t % 2]
            else:
                kt = kc.T
            s = jnp.dot(qblk[rs, :], kt, preferred_element_type=jnp.float32)
            pos = lax.broadcasted_iota(jnp.int32, (1, CHUNK), 1) + (base + lo)
            s = jnp.where(pos < ln[rs, :], s, MASKED)
            sbuf[g % 2, rs, lo:lo + CHUNK] = s
            return jnp.maximum(m, fold(s, jnp.maximum))

        n_pairs = GROUP // 2
        pair_rows = 2 * n_heads

        def no_max():
            return [jnp.full((pair_rows, hd), MASKED, jnp.float32) for _ in range(n_pairs)]

        def scores(g, ln):
            ms = no_max()
            for lo in range(0, seq, CHUNK):
                ms = [score_tile(g, t, lo, ln, ms[t], t < n_pairs - 1) for t in range(n_pairs)]
            return ms

        def weights(g, lo, size, mu):
            w = jnp.exp2((sbuf[g % 2, :, lo:lo + size] - mu) * exp_c)
            return w.astype(jnp.bfloat16), fold(w, jnp.add)

        def weighted(g, r, wt, lo, size):
            vc = jnp.concatenate([vb[g % RING, r + i, lo:lo + size, :] for i in range(2)], axis=1)
            o = jnp.dot(wt, vc, preferred_element_type=jnp.float32)
            return jnp.concatenate([o[:n_heads, :hd], o[n_heads:, hd:]], axis=0)

        def attend(g, mu, ln):
            outs = [None] * n_pairs
            ms = no_max()
            l = jnp.zeros((hd, hd), jnp.float32)
            for lo in range(0, seq, CHUNK):
                wt, part = weights(g, lo, CHUNK, mu)
                l = l + part
                for t in range(n_pairs):
                    if ln is not None:
                        ms[t] = score_tile(g + 1, t, lo, ln, ms[t])
                    o = weighted(g, 2 * t, wt[t * pair_rows:(t + 1) * pair_rows, :], lo, CHUNK)
                    outs[t] = o if outs[t] is None else outs[t] + o
            for t in range(n_pairs):
                oacc[t * pair_rows:(t + 1) * pair_rows, :] = outs[t]
            return ms, l

        def keep_max(g, ms):
            m = jnp.concatenate(ms, axis=0)
            mrow[g % 2] = jnp.broadcast_to(jnp.max(m, axis=1, keepdims=True), (hd, hd))

        def stat_rows(g, l):
            l_col = jnp.sum(l, axis=1, keepdims=True)
            return jnp.where(lane == 0, mrow[g % 2], jnp.where(lane == 1, l_col, 0.0)).T[:8, :]

        def p_copy(g, d):
            return pltpu.make_async_remote_copy(
                src_ref=psend.at[d, g], dst_ref=prec.at[g, d], send_sem=ps_sem.at[d],
                recv_sem=pr_sem.at[g], device_id=(bx, peers[d]), device_id_type=MESH)

        def send_part(g, l):
            for h in range(n_heads):
                k, hh = h // heads_local, h % heads_local
                psend[k, g, hh * GROUP:(hh + 1) * GROUP, :] = oacc[pl.ds(h, GROUP, stride=n_heads), :]
            ml = stat_rows(g, l)
            for k in range(4):
                psend[k, g, prow:prow + 8, :] = ml
            for d in far_first:
                p_copy(g, d).start()

        def t_copy(c, d):
            return pltpu.make_async_remote_copy(
                src_ref=tsend.at[d, c], dst_ref=trec.at[c, d], send_sem=ts_sem.at[d],
                recv_sem=tr_sem.at[c], device_id=(bx, peers[d]), device_id_type=MESH)

        def send_piece(c, ml):
            for h in range(n_heads):
                k, hh = h // heads_local, h % heads_local
                tsend[k, c, hh * PIECE:(hh + 1) * PIECE, :] = (
                    oacc[pl.ds(c * PIECE * n_heads + h, PIECE, stride=n_heads), :])
            for k in range(4):
                tsend[k, c, piece_rows:piece_rows + 8, :] = ml
            for d in far_first:
                t_copy(c, d).start()

        def picks(nr, r0):
            row = lax.broadcasted_iota(jnp.int32, (heads_local * nr, hd), 0)
            at = (r0 + row % nr) * n_heads + row // nr
            lane_p = lax.broadcasted_iota(jnp.int32, (heads_local * nr, hd), 1)
            return [lane_p == at + d * heads_local for d in range(4)]

        def combine_rows(parts, row0, nr, picked):
            n = heads_local * nr
            rs = slice(row0, row0 + nr)

            def to_col(d, row):
                return jnp.sum(jnp.where(picked[d], row, 0.0), axis=1, keepdims=True)

            s_new = jnp.concatenate([snew[h, rs, :] for h in range(heads_local)], axis=0)
            ms = [to_col(d, p[n:n + 1, :]) for d, p in enumerate(parts)]
            ls = [to_col(d, p[n + 1:n + 2, :]) for d, p in enumerate(parts)]
            top = s_new
            for m in ms:
                top = jnp.maximum(top, m)
            f_new = jnp.exp2((s_new - top) * exp_c)
            den = f_new
            num = f_new * jnp.concatenate([vnf[rs, :]] * heads_local, axis=0)
            for p, m, l in zip(parts, ms, ls):
                f = jnp.exp2((m - top) * exp_c)
                den = den + f * l
                num = num + f * p[:n, :]
            o = num / den
            for h in range(heads_local):
                attn[rs, h * hd:(h + 1) * hd] = o[h * nr:(h + 1) * nr, :]

        def combine(g):
            parts = [prec[g, d] for d in range(3)] + [psend[3, g]]
            combine_rows(parts, g * GROUP, GROUP, picks(GROUP, 0))

        def combine_piece(c):
            pltpu.make_async_copy(trec.at[c], trec.at[c], tr_sem.at[c]).wait()
            parts = [trec[c, d] for d in range(3)] + [tsend[3, c]]
            combine_rows(parts, last * GROUP + c * PIECE, PIECE, picks(PIECE, c * PIECE))

        def p_wait(g):
            pltpu.make_async_copy(prec.at[g], prec.at[g], pr_sem.at[g]).wait()

        y_batches = []

        def y_copy(b, g0, ng, d):
            sl = pl.ds(g0 * GROUP, ng * GROUP)
            return pltpu.make_async_remote_copy(
                src_ref=ysend.at[peers[d], sl], dst_ref=y_out.at[d, sl], send_sem=ys_sem.at[d],
                recv_sem=yr_sem.at[b], device_id=(bx, peers[d]), device_id_type=MESH)

        def project(g0, ng):
            b = len(y_batches)
            y_batches.append((b, g0, ng))
            sl = slice(g0 * GROUP, (g0 + ng) * GROUP)
            yp = jnp.dot(attn[sl, :].astype(jnp.bfloat16), wo[...], preferred_element_type=jnp.float32)
            for k in range(4):
                ysend[k, sl, :] = yp[:, k * q_cols:(k + 1) * q_cols]
            for d in far_first:
                y_copy(b, g0, ng, d).start()
            y_out[3, sl, :] = ysend[me, sl, :]

        def finish(b, g0, ng):
            sl = pl.ds(g0 * GROUP, ng * GROUP)
            pltpu.make_async_copy(y_out.at[0:3, sl], y_out.at[0:3, sl], yr_sem.at[b]).wait()

        q_wait(0)
        build_q(0)
        k_copy(0).wait()
        keep_max(0, scores(0, lens_col(0)))

        def shift(g):
            return jnp.where(lens_col(g) > base, mrow[g % 2, :, 0:1], 0.0)

        for g in range(last - 1):
            if g + 3 < n_groups:
                k_copy(g + 3).start()
            if g + 2 < last:
                v_copy(g + 2).start()
            if g + 2 == last:
                for c in range(n_pieces):
                    v_tail(c).start()
            q_wait(g + 1)
            if g >= 2:
                p_wait(g - 2)
            if g == 3:
                ins[5].wait()
            k_copy(g + 1).wait()
            v_copy(g).wait()
            build_q(g + 1)
            ms, l = attend(g, shift(g), lens_col(g + 1))
            keep_max(g + 1, ms)
            send_part(g, l)
            if g >= 2:
                combine(g - 2)
            if g in Y_BATCHES:
                project(*Y_BATCHES[g])

        pre = last - 1
        q_wait(last)
        k_copy(last).wait()
        build_q(last)
        keep_max(last, scores(last, lens_col(last)))
        v_copy(pre).wait()
        mu = shift(last)
        pre_l = attend(pre, shift(pre), None)[1]
        l = jnp.zeros((hd, hd), jnp.float32)
        for lo in range(0, seq, CHUNK):
            wt, part = weights(last, lo, CHUNK, mu)
            wts[:, lo:lo + CHUNK] = wt
            l = l + part
        ml = stat_rows(last, l)
        send_part(pre, pre_l)
        for c in range(n_pieces):
            v_tail(c).wait()
            for r in range(c * PIECE, (c + 1) * PIECE, 2):
                rs = slice(r * n_heads, (r + 2) * n_heads)
                oacc[rs, :] = weighted(last, r, wts[rs, :], 0, seq)
            send_piece(c, ml)
        done = max(g0 + ng for g0, ng in Y_BATCHES.values())
        for g in (pre - 2, pre - 1):
            p_wait(g)
            combine(g)
        project(done, pre - done)
        p_wait(pre)
        combine(pre)
        project(pre, 1)
        for c in range(n_pieces):
            combine_piece(c)
        project(last, 1)
        for b in y_batches:
            finish(*b)
        for d in range(3):
            pltpu.make_async_copy(qown, qown, qs_sem.at[d]).wait()
            pltpu.make_async_copy(psend.at[d], psend.at[d], ps_sem.at[d]).wait()
            pltpu.make_async_copy(tsend.at[d], tsend.at[d], ts_sem.at[d]).wait()
            pltpu.make_async_copy(ysend.at[d], ysend.at[d], ys_sem.at[d]).wait()

    f32, bf16 = jnp.float32, jnp.bfloat16
    dma = pltpu.SemaphoreType.DMA
    n_b = len(Y_BATCHES) + 3
    scratch = [
        pltpu.VMEM((rows, embed), bf16), pltpu.VMEM((embed, q_cols), bf16), pltpu.VMEM((2, embed, hd), bf16),
        pltpu.VMEM((q_cols, embed), bf16), pltpu.SMEM((rows,), jnp.int32),
        pltpu.VMEM((RING, GROUP, seq, hd), bf16), pltpu.VMEM((RING, GROUP, seq, hd), bf16),
        pltpu.VMEM((n_groups, GROUP, q_cols), f32), pltpu.VMEM((n_groups, 3, GROUP, q_cols), f32),
        pltpu.VMEM((hd, hd), f32), pltpu.VMEM((hd, 2 * hd), bf16), pltpu.VMEM((2, 2 * hd, CHUNK), bf16),
        pltpu.VMEM((2, hd, seq), f32), pltpu.VMEM((hd, hd), f32), pltpu.VMEM((2, hd, hd), f32),
        pltpu.VMEM((rows, hd), f32),
        pltpu.VMEM((heads_local, rows, hd), f32),
        pltpu.VMEM((hd, seq), bf16),
        pltpu.VMEM((4, last, prow + 8, hd), f32), pltpu.VMEM((last, 3, prow + 8, hd), f32),
        pltpu.VMEM((4, n_pieces, piece_rows + 8, hd), f32), pltpu.VMEM((n_pieces, 3, piece_rows + 8, hd), f32),
        pltpu.VMEM((rows, q_cols), f32), pltpu.VMEM((4, rows, q_cols), f32),
        dma((6,)), dma((RING,)), dma((RING,)), dma((n_pieces,)), dma((3,)), dma((n_groups,)),
        dma((3,)), dma((last,)), dma((3,)), dma((n_pieces,)), dma((3,)), dma((n_b,)),
    ]
    return kernel, scratch


def store_kernel(y_ref, k_ref, v_ref, yo_ref, ko_ref, vo_ref, y16, sem):
    y16[...] = (y_ref[3] + y_ref[0] + y_ref[1] + y_ref[2]).astype(y16.dtype)
    writes = [pltpu.make_async_copy(a, b, sem.at[i])
              for i, (a, b) in enumerate(((y16, yo_ref), (k_ref, ko_ref), (v_ref, vo_ref)))]
    for w in writes:
        w.start()
    for w in writes:
        w.wait()


def solution(mesh):
    def local_step(hidden, w_query, w_key, w_value, w_out, k_cache, v_cache, lengths):
        rows, embed = hidden.shape
        hd = w_key.shape[1]
        seq = k_cache.shape[1]
        heads_local = w_query.shape[1] // hd
        q_cols = heads_local * hd
        kernel, scratch = make_kernel(rows, embed, seq, heads_local, hd)
        any_spec = pl.BlockSpec(memory_space=pl.ANY)
        vmem_spec = pl.BlockSpec(memory_space=pltpu.VMEM)
        outs = (jax.ShapeDtypeStruct((rows, q_cols), jnp.bfloat16),
                jax.ShapeDtypeStruct((rows, hd), jnp.bfloat16),
                jax.ShapeDtypeStruct((rows, hd), jnp.bfloat16))
        raw = pl.pallas_call(
            kernel,
            out_shape=tuple(pltpu.VMEM(sh, dt) for sh, dt in (((4, rows, q_cols), jnp.float32),
                                                              ((rows, hd), jnp.bfloat16), ((rows, hd), jnp.bfloat16))),
            in_specs=[any_spec] * 8,
            out_specs=(vmem_spec,) * 3,
            scratch_shapes=scratch,
            compiler_params=pltpu.CompilerParams(
                collective_id=0, has_side_effects=True, vmem_limit_bytes=66300000),
            name="mqa_decode",
        )(hidden, w_query, w_key, w_value, w_out, k_cache, v_cache, lengths)
        return pl.pallas_call(
            store_kernel,
            out_shape=outs,
            in_specs=[vmem_spec] * 3,
            out_specs=(any_spec,) * 3,
            scratch_shapes=[pltpu.VMEM(outs[0].shape, outs[0].dtype), pltpu.SemaphoreType.DMA((3,))],
            name="store_outputs",
        )(*[pltpu.with_memory_space_constraint(r, pltpu.VMEM) for r in raw])

    return jax.shard_map(
        local_step,
        mesh=mesh,
        in_specs=(P('bx', None), P(None, 'sq'), P(None, None), P(None, None), P('sq', None),
                  P('bx', 'sq', None), P('bx', 'sq', None), P('bx')),
        out_specs=(P('bx', 'sq'), P('bx', None), P('bx', None)),
        check_vma=False,
    )
```

```python
import math
import jax
import jax.numpy as jnp
from jax import lax
from jax.experimental import pallas as pl
from jax.experimental.pallas import tpu as pltpu
from jax.sharding import PartitionSpec as P

ROPE_BASE = 10000.0
GROUP = 8
RING = 3
CHUNK = 512
PIECE = 4
MASKED = -3e38
MESH = pl.DeviceIdType.MESH
Y_BATCHES = {3: (0, 2), 4: (2, 1)}


def make_kernel(rows, embed, seq, heads_local, hd):
    n_groups = rows // GROUP
    n_heads = 4 * heads_local
    assert n_heads * GROUP == hd and hd == 128
    q_cols = heads_local * hd
    last = n_groups - 1
    exp_c = hd ** -0.5 * math.log2(math.e)
    n_pieces = GROUP // PIECE
    piece_rows = heads_local * PIECE
    half = hd // 2
    freqs = [ROPE_BASE ** (-2.0 * i / hd) for i in range(half)]
    prow = heads_local * GROUP

    def kernel(hid_hbm, wq_hbm, wk_hbm, wv_hbm, wo_hbm, k_hbm, v_hbm, len_hbm,
               y_out, yl_out, kn_out, vn_out,
               hid, wq, wkv, wo, lens_s, kb, vb, qown, qrec, qmat, qblk, k_turn, sbuf, oacc, mrow,
               vnf, snew, wts, psend, prec, tsend, trec, attn, ysend, ylsend,
               in_sem, ksem, vsem, tsem, qs_sem, qr_sem, ps_sem, pr_sem, ts_sem, tr_sem, yls_sem, ylr_sem, ys_sem, yr_sem):
        bx = lax.axis_index('bx')
        me = lax.axis_index('sq')
        chip, core = me // 2, me % 2
        peers = [chip * 2 + (1 - core), (1 - chip) * 2 + core, (1 - chip) * 2 + (1 - core)]
        far_first = (1, 2, 0)
        base = me * seq

        def cp(src, dst, sem):
            return pltpu.make_async_copy(src, dst, sem)

        def k_copy(g):
            return cp(k_hbm.at[pl.ds(g * GROUP, GROUP)], kb.at[g % RING], ksem.at[g % RING])

        def v_copy(g):
            return cp(v_hbm.at[pl.ds(g * GROUP, GROUP)], vb.at[g % RING], vsem.at[g % RING])

        def v_tail(c):
            r0 = last * GROUP + c * PIECE
            return cp(v_hbm.at[r0:r0 + PIECE], vb.at[last % RING, c * PIECE:(c + 1) * PIECE], tsem.at[c])

        ins = [cp(len_hbm, lens_s, in_sem.at[0]), cp(hid_hbm, hid, in_sem.at[1]), cp(wq_hbm, wq, in_sem.at[2]),
               cp(wk_hbm, wkv.at[0], in_sem.at[3]), cp(wv_hbm, wkv.at[1], in_sem.at[4]), cp(wo_hbm, wo, in_sem.at[5])]
        for c in ins[:5]:
            c.start()
        k_copy(0).start()
        k_copy(1).start()
        v_copy(0).start()

        barrier = pltpu.get_barrier_semaphore()
        for p in peers:
            pl.semaphore_signal(barrier, inc=1, device_id=(bx, p), device_id_type=MESH)

        k_copy(2).start()
        v_copy(1).start()
        ins[5].start()

        lane = lax.broadcasted_iota(jnp.int32, (1, hd), 1)
        lane_i = lane % half
        freq = jnp.zeros((1, hd), jnp.float32)
        for i in range(half):
            freq = jnp.where(lane_i == i, jnp.float32(freqs[i]), freq)
        ins[0].wait()
        sub = lax.broadcasted_iota(jnp.int32, (GROUP, 1), 0)
        pos_rows = []
        for g in range(n_groups):
            t = jnp.zeros((GROUP, 1), jnp.int32)
            for r in range(GROUP):
                t = jnp.where(sub == r, lens_s[g * GROUP + r], t)
            pos_rows.append(t)
        t_col = jnp.concatenate(pos_rows, axis=0).astype(jnp.float32)
        ang = t_col * freq
        cos_t = jnp.cos(ang)
        sin_t = jnp.where(lane < half, -1.0, 1.0) * jnp.sin(ang)

        def rope(x):
            return x * cos_t + pltpu.roll(x, half, 1) * sin_t

        ins[1].wait()
        ins[2].wait()
        qp = jnp.dot(hid[...], wq[...], preferred_element_type=jnp.float32)
        for h in range(heads_local):
            cs = slice(h * hd, (h + 1) * hd)
            q_h = rope(qp[:, cs]).astype(jnp.bfloat16).astype(jnp.float32)
            qown[:, :, cs] = q_h.reshape(n_groups, GROUP, hd)
        pl.semaphore_wait(barrier, 3)

        def q_copy(g, d):
            return pltpu.make_async_remote_copy(
                src_ref=qown.at[g], dst_ref=qrec.at[g, d], send_sem=qs_sem.at[d],
                recv_sem=qr_sem.at[g], device_id=(bx, peers[d]), device_id_type=MESH)

        for g in range(n_groups):
            for d in far_first:
                q_copy(g, d).start()

        ins[3].wait()
        ins[4].wait()
        kn = rope(jnp.dot(hid[...], wkv[0], preferred_element_type=jnp.float32)).astype(jnp.bfloat16)
        vn = jnp.dot(hid[...], wkv[1], preferred_element_type=jnp.float32).astype(jnp.bfloat16)
        kn_out[...] = kn
        vn_out[...] = vn
        knf = kn.astype(jnp.float32)
        vnf[...] = vn.astype(jnp.float32)
        for h in range(heads_local):
            q_h = qown[:, :, h * hd:(h + 1) * hd].reshape(rows, hd)
            s_h = jnp.sum(q_h * knf, axis=1, keepdims=True)
            snew[h] = jnp.broadcast_to(s_h, (rows, hd))

        def per_row(g, vals):
            return jnp.concatenate([jnp.full((n_heads, 1), vals(g * GROUP + r), jnp.int32) for r in range(GROUP)], axis=0)

        def lens_col(g):
            return per_row(g, lambda b: lens_s[b])

        qblk[...] = jnp.zeros_like(qblk)

        def q_wait(g):
            pltpu.make_async_copy(qrec.at[g], qrec.at[g], qr_sem.at[g]).wait()

        def build_q(g):
            for s in range(4):
                for h in range(heads_local):
                    cs = slice(h * hd, (h + 1) * hd)
                    blk = qown[g, :, cs] if s == 3 else qrec[g, s, :, cs]
                    qmat[pl.ds(s * heads_local + h, GROUP, stride=n_heads), :] = blk
            for r in range(GROUP):
                rs = slice(r * n_heads, (r + 1) * n_heads)
                qblk[rs, (r % 2) * hd:(r % 2 + 1) * hd] = qmat[rs, :].astype(jnp.bfloat16)

        def fold(x, op):
            out = x[:, :hd]
            for i in range(1, x.shape[1] // hd):
                out = op(out, x[:, i * hd:(i + 1) * hd])
            return out

        def score_tile(g, t, lo, ln, m, turn=True):
            rs = slice(2 * t * n_heads, (2 * t + 2) * n_heads)
            kc = jnp.concatenate([kb[g % RING, 2 * t + i, lo:lo + CHUNK, :] for i in range(2)], axis=1)
            if turn:
                k_turn[t % 2] = kc.T
                kt = k_turn[t % 2]
            else:
                kt = kc.T
            s = jnp.dot(qblk[rs, :], kt, preferred_element_type=jnp.float32)
            pos = lax.broadcasted_iota(jnp.int32, (1, CHUNK), 1) + (base + lo)
            s = jnp.where(pos < ln[rs, :], s, MASKED)
            sbuf[g % 2, rs, lo:lo + CHUNK] = s
            return jnp.maximum(m, fold(s, jnp.maximum))

        n_pairs = GROUP // 2
        pair_rows = 2 * n_heads

        def no_max():
            return [jnp.full((pair_rows, hd), MASKED, jnp.float32) for _ in range(n_pairs)]

        def scores(g, ln):
            ms = no_max()
            for lo in range(0, seq, CHUNK):
                ms = [score_tile(g, t, lo, ln, ms[t], t < n_pairs - 1) for t in range(n_pairs)]
            return ms

        def weights(g, lo, size, mu):
            w = jnp.exp2((sbuf[g % 2, :, lo:lo + size] - mu) * exp_c)
            return w.astype(jnp.bfloat16), fold(w, jnp.add)

        def weighted(g, r, wt, lo, size):
            vc = jnp.concatenate([vb[g % RING, r + i, lo:lo + size, :] for i in range(2)], axis=1)
            o = jnp.dot(wt, vc, preferred_element_type=jnp.float32)
            return jnp.concatenate([o[:n_heads, :hd], o[n_heads:, hd:]], axis=0)

        def attend(g, mu, ln):
            outs = [None] * n_pairs
            ms = no_max()
            l = jnp.zeros((hd, hd), jnp.float32)
            for lo in range(0, seq, CHUNK):
                wt, part = weights(g, lo, CHUNK, mu)
                l = l + part
                for t in range(n_pairs):
                    if ln is not None:
                        ms[t] = score_tile(g + 1, t, lo, ln, ms[t])
                    o = weighted(g, 2 * t, wt[t * pair_rows:(t + 1) * pair_rows, :], lo, CHUNK)
                    outs[t] = o if outs[t] is None else outs[t] + o
            for t in range(n_pairs):
                oacc[t * pair_rows:(t + 1) * pair_rows, :] = outs[t]
            return ms, l

        def keep_max(g, ms):
            m = jnp.concatenate(ms, axis=0)
            mrow[g % 2] = jnp.broadcast_to(jnp.max(m, axis=1, keepdims=True), (hd, hd))

        def stat_rows(g, l):
            l_col = jnp.sum(l, axis=1, keepdims=True)
            return jnp.where(lane == 0, mrow[g % 2], jnp.where(lane == 1, l_col, 0.0)).T[:8, :]

        def p_copy(g, d):
            return pltpu.make_async_remote_copy(
                src_ref=psend.at[d, g], dst_ref=prec.at[g, d], send_sem=ps_sem.at[d],
                recv_sem=pr_sem.at[g], device_id=(bx, peers[d]), device_id_type=MESH)

        def send_part(g, l):
            for h in range(n_heads):
                k, hh = h // heads_local, h % heads_local
                psend[k, g, hh * GROUP:(hh + 1) * GROUP, :] = oacc[pl.ds(h, GROUP, stride=n_heads), :]
            ml = stat_rows(g, l)
            for k in range(4):
                psend[k, g, prow:prow + 8, :] = ml
            for d in far_first:
                p_copy(g, d).start()

        def t_copy(c, d):
            n = piece_rows + (8 if c == 0 else 0)
            return pltpu.make_async_remote_copy(
                src_ref=tsend.at[d, c, 0:n], dst_ref=trec.at[c, d, 0:n], send_sem=ts_sem.at[d, c],
                recv_sem=tr_sem.at[c], device_id=(bx, peers[d]), device_id_type=MESH)

        def send_piece(c, ml):
            for h in range(n_heads):
                k, hh = h // heads_local, h % heads_local
                tsend[k, c, hh * PIECE:(hh + 1) * PIECE, :] = (
                    oacc[pl.ds(c * PIECE * n_heads + h, PIECE, stride=n_heads), :])
            if c == 0:
                for k in range(4):
                    tsend[k, c, piece_rows:piece_rows + 8, :] = ml
            for d in far_first:
                t_copy(c, d).start()

        def picks(nr, r0):
            row = lax.broadcasted_iota(jnp.int32, (heads_local * nr, hd), 0)
            at = (r0 + row % nr) * n_heads + row // nr
            lane_p = lax.broadcasted_iota(jnp.int32, (heads_local * nr, hd), 1)
            return [lane_p == at + d * heads_local for d in range(4)]

        def combine_rows(parts, row0, nr, picked):
            n = heads_local * nr
            rs = slice(row0, row0 + nr)

            def to_col(d, row):
                return jnp.sum(jnp.where(picked[d], row, 0.0), axis=1, keepdims=True)

            s_new = jnp.concatenate([snew[h, rs, :] for h in range(heads_local)], axis=0)
            ms = [to_col(d, p[n:n + 1, :]) for d, p in enumerate(parts)]
            ls = [to_col(d, p[n + 1:n + 2, :]) for d, p in enumerate(parts)]
            top = s_new
            for m in ms:
                top = jnp.maximum(top, m)
            f_new = jnp.exp2((s_new - top) * exp_c)
            den = f_new
            num = f_new * jnp.concatenate([vnf[rs, :]] * heads_local, axis=0)
            for p, m, l in zip(parts, ms, ls):
                f = jnp.exp2((m - top) * exp_c)
                den = den + f * l
                num = num + f * p[:n, :]
            o = num / den
            for h in range(heads_local):
                attn[rs, h * hd:(h + 1) * hd] = o[h * nr:(h + 1) * nr, :]

        def combine(g):
            parts = [prec[g, d] for d in range(3)] + [psend[3, g]]
            combine_rows(parts, g * GROUP, GROUP, picks(GROUP, 0))

        def combine_piece(c):
            n = piece_rows + (8 if c == 0 else 0)
            pltpu.make_async_copy(trec.at[c, :, 0:n], trec.at[c, :, 0:n], tr_sem.at[c]).wait()
            stats = slice(piece_rows, piece_rows + 8)
            parts = [jnp.concatenate([trec[c, d, 0:piece_rows, :], trec[0, d, stats, :]], axis=0) for d in range(3)]
            parts.append(jnp.concatenate([tsend[3, c, 0:piece_rows, :], tsend[3, 0, stats, :]], axis=0))
            combine_rows(parts, last * GROUP + c * PIECE, PIECE, picks(PIECE, c * PIECE))

        def p_wait(g):
            pltpu.make_async_copy(prec.at[g], prec.at[g], pr_sem.at[g]).wait()

        y_batches = []

        def y_copy(b, g0, ng, d):
            sl = pl.ds(g0 * GROUP, ng * GROUP)
            return pltpu.make_async_remote_copy(
                src_ref=ysend.at[peers[d], sl], dst_ref=y_out.at[d, sl], send_sem=ys_sem.at[d],
                recv_sem=yr_sem.at[b], device_id=(bx, peers[d]), device_id_type=MESH)

        def project(g0, ng):
            b = len(y_batches)
            y_batches.append((b, g0, ng))
            sl = slice(g0 * GROUP, (g0 + ng) * GROUP)
            yp = jnp.dot(attn[sl, :].astype(jnp.bfloat16), wo[...], preferred_element_type=jnp.float32)
            for k in range(4):
                ysend[k, sl, :] = yp[:, k * q_cols:(k + 1) * q_cols]
            for d in far_first:
                y_copy(b, g0, ng, d).start()
            y_out[3, sl, :] = ysend[me, sl, :]

        def yl_copy(c, d):
            return pltpu.make_async_remote_copy(
                src_ref=ylsend.at[peers[d], c], dst_ref=yl_out.at[d, c], send_sem=yls_sem.at[d],
                recv_sem=ylr_sem.at[c], device_id=(bx, peers[d]), device_id_type=MESH)

        def project_piece(c):
            r0 = last * GROUP + c * PIECE
            lhs = attn[r0:r0 + PIECE, :].astype(jnp.bfloat16)
            for side, near in ((1 - chip, False), (chip, True)):
                col = pl.multiple_of(side * 2 * q_cols, 2 * q_cols)
                yp = jnp.dot(lhs, wo[:, pl.ds(col, 2 * q_cols)], preferred_element_type=jnp.float32)
                for k in range(2):
                    ylsend[side * 2 + k, c] = yp[:, k * q_cols:(k + 1) * q_cols]
                for d in ((0,) if near else (1, 2)):
                    yl_copy(c, d).start()
            yl_out[3, c] = ylsend[me, c]

        def finish(b, g0, ng):
            sl = pl.ds(g0 * GROUP, ng * GROUP)
            pltpu.make_async_copy(y_out.at[0:3, sl], y_out.at[0:3, sl], yr_sem.at[b]).wait()

        q_wait(0)
        build_q(0)
        k_copy(0).wait()
        keep_max(0, scores(0, lens_col(0)))

        def shift(g):
            return jnp.where(lens_col(g) > base, mrow[g % 2, :, 0:1], 0.0)

        for g in range(last - 1):
            if g + 3 < n_groups:
                k_copy(g + 3).start()
            if g + 2 < last:
                v_copy(g + 2).start()
            if g + 2 == last:
                for c in range(n_pieces):
                    v_tail(c).start()
            q_wait(g + 1)
            if g >= 2:
                p_wait(g - 2)
            if g == 3:
                ins[5].wait()
            k_copy(g + 1).wait()
            v_copy(g).wait()
            build_q(g + 1)
            ms, l = attend(g, shift(g), lens_col(g + 1))
            keep_max(g + 1, ms)
            send_part(g, l)
            if g >= 2:
                combine(g - 2)
            if g in Y_BATCHES:
                project(*Y_BATCHES[g])

        pre = last - 1
        q_wait(last)
        k_copy(last).wait()
        build_q(last)
        keep_max(last, scores(last, lens_col(last)))
        v_copy(pre).wait()
        mu = shift(last)
        pre_l = attend(pre, shift(pre), None)[1]
        l = jnp.zeros((hd, hd), jnp.float32)
        for lo in range(0, seq, CHUNK):
            wt, part = weights(last, lo, CHUNK, mu)
            wts[:, lo:lo + CHUNK] = wt
            l = l + part
        ml = stat_rows(last, l)
        send_part(pre, pre_l)
        for c in range(n_pieces):
            v_tail(c).wait()
            for r in range(c * PIECE, (c + 1) * PIECE, 2):
                rs = slice(r * n_heads, (r + 2) * n_heads)
                oacc[rs, :] = weighted(last, r, wts[rs, :], 0, seq)
            send_piece(c, ml)
        done = max(g0 + ng for g0, ng in Y_BATCHES.values())
        for g in range(pre - 2, last):
            p_wait(g)
            combine(g)
            project(done, g + 1 - done)
            done = g + 1
        for c in range(n_pieces):
            combine_piece(c)
            project_piece(c)
        for b in y_batches:
            finish(*b)
        for c in range(n_pieces):
            pltpu.make_async_copy(yl_out.at[0:3, c], yl_out.at[0:3, c], ylr_sem.at[c]).wait()
        for d in range(3):
            pltpu.make_async_copy(qown, qown, qs_sem.at[d]).wait()
            pltpu.make_async_copy(psend.at[d], psend.at[d], ps_sem.at[d]).wait()
            for c in range(n_pieces):
                t_copy(c, d).wait_send()
            pltpu.make_async_copy(ysend.at[d], ysend.at[d], ys_sem.at[d]).wait()
            pltpu.make_async_copy(ylsend.at[d], ylsend.at[d], yls_sem.at[d]).wait()

    f32, bf16 = jnp.float32, jnp.bfloat16
    dma = pltpu.SemaphoreType.DMA
    n_b = len(Y_BATCHES) + 3
    scratch = [
        pltpu.VMEM((rows, embed), bf16), pltpu.VMEM((embed, q_cols), bf16), pltpu.VMEM((2, embed, hd), bf16),
        pltpu.VMEM((q_cols, embed), bf16), pltpu.SMEM((rows,), jnp.int32),
        pltpu.VMEM((RING, GROUP, seq, hd), bf16), pltpu.VMEM((RING, GROUP, seq, hd), bf16),
        pltpu.VMEM((n_groups, GROUP, q_cols), f32), pltpu.VMEM((n_groups, 3, GROUP, q_cols), f32),
        pltpu.VMEM((hd, hd), f32), pltpu.VMEM((hd, 2 * hd), bf16), pltpu.VMEM((2, 2 * hd, CHUNK), bf16),
        pltpu.VMEM((2, hd, seq), f32), pltpu.VMEM((hd, hd), f32), pltpu.VMEM((2, hd, hd), f32),
        pltpu.VMEM((rows, hd), f32),
        pltpu.VMEM((heads_local, rows, hd), f32),
        pltpu.VMEM((hd, seq), bf16),
        pltpu.VMEM((4, last, prow + 8, hd), f32), pltpu.VMEM((last, 3, prow + 8, hd), f32),
        pltpu.VMEM((4, n_pieces, piece_rows + 8, hd), f32), pltpu.VMEM((n_pieces, 3, piece_rows + 8, hd), f32),
        pltpu.VMEM((rows, q_cols), f32), pltpu.VMEM((4, last * GROUP, q_cols), f32),
        pltpu.VMEM((4, n_pieces, PIECE, q_cols), f32),
        dma((6,)), dma((RING,)), dma((RING,)), dma((n_pieces,)), dma((3,)), dma((n_groups,)),
        dma((3,)), dma((last,)), dma((3, n_pieces)), dma((n_pieces,)), dma((3,)), dma((n_pieces,)), dma((3,)), dma((n_b,)),
    ]
    return kernel, scratch


def store_kernel(y_ref, yl_ref, k_ref, v_ref, yo_ref, ko_ref, vo_ref, y16, sem):
    most = y_ref.shape[1]
    y16[:most, :] = (y_ref[3] + y_ref[0] + y_ref[1] + y_ref[2]).astype(y16.dtype)
    tail = [yl_ref[3, c] + yl_ref[0, c] + yl_ref[1, c] + yl_ref[2, c] for c in range(yl_ref.shape[1])]
    y16[most:, :] = jnp.concatenate(tail, axis=0).astype(y16.dtype)
    writes = [pltpu.make_async_copy(a, b, sem.at[i])
              for i, (a, b) in enumerate(((y16, yo_ref), (k_ref, ko_ref), (v_ref, vo_ref)))]
    for w in writes:
        w.start()
    for w in writes:
        w.wait()


def solution(mesh):
    def local_step(hidden, w_query, w_key, w_value, w_out, k_cache, v_cache, lengths):
        rows, embed = hidden.shape
        hd = w_key.shape[1]
        seq = k_cache.shape[1]
        heads_local = w_query.shape[1] // hd
        q_cols = heads_local * hd
        kernel, scratch = make_kernel(rows, embed, seq, heads_local, hd)
        any_spec = pl.BlockSpec(memory_space=pl.ANY)
        vmem_spec = pl.BlockSpec(memory_space=pltpu.VMEM)
        outs = (jax.ShapeDtypeStruct((rows, q_cols), jnp.bfloat16),
                jax.ShapeDtypeStruct((rows, hd), jnp.bfloat16),
                jax.ShapeDtypeStruct((rows, hd), jnp.bfloat16))
        raw = pl.pallas_call(
            kernel,
            out_shape=tuple(pltpu.VMEM(sh, dt) for sh, dt in (((4, rows - GROUP, q_cols), jnp.float32),
                                                              ((4, GROUP // PIECE, PIECE, q_cols), jnp.float32),
                                                              ((rows, hd), jnp.bfloat16), ((rows, hd), jnp.bfloat16))),
            in_specs=[any_spec] * 8,
            out_specs=(vmem_spec,) * 4,
            scratch_shapes=scratch,
            compiler_params=pltpu.CompilerParams(
                collective_id=0, has_side_effects=True, vmem_limit_bytes=66300000),
            name="mqa_decode",
        )(hidden, w_query, w_key, w_value, w_out, k_cache, v_cache, lengths)
        return pl.pallas_call(
            store_kernel,
            out_shape=outs,
            in_specs=[vmem_spec] * 4,
            out_specs=(any_spec,) * 3,
            scratch_shapes=[pltpu.VMEM(outs[0].shape, outs[0].dtype), pltpu.SemaphoreType.DMA((3,))],
            name="store_outputs",
        )(*[pltpu.with_memory_space_constraint(r, pltpu.VMEM) for r in raw])

    return jax.shard_map(
        local_step,
        mesh=mesh,
        in_specs=(P('bx', None), P(None, 'sq'), P(None, None), P(None, None), P('sq', None),
                  P('bx', 'sq', None), P('bx', 'sq', None), P('bx')),
        out_specs=(P('bx', 'sq'), P('bx', None), P('bx', None)),
        check_vma=False,
    )
```
